32 devices in a mesh: slab: 2 (over y), date: 8 (over z, x), tile: 1, sub: 2 (over core).
Axes of the slice: x: 2, y: 2, z: 4, core: 2. Of those that a mesh axis runs over, the one named last changes fastest.
Arguments:
- slc: bfloat16 [2, 100, 128, 512], P(None, None, 'date', ('slab', 'tile', 'sub')), parts along dimension 3, may hold values from -300 to 300, as said below
- usable: int32 [100, 128, 512], P(None, 'date', ('slab', 'tile', 'sub')), parts along dimension 2, may hold values 0 or 1
Outputs:
- coherence: bfloat16 [2, 4, 8, 16, 128, 128], P(None, ('slab', 'tile', 'sub'), 'date'), parts along dimension 1
- linked: float32 [2, 128, 512], P(None, 'date', ('slab', 'tile', 'sub')), parts along dimension 2
The draws below stay inside these ranges and needn't reach their ends.
There are 2 independent parts, one for each index of `slab`. The reference program is written for one: setup_inputs(seed, part) draws one part's arguments, and reference() takes and returns one part's arrays. A program takes and returns all parts, laid end to end along the dimension named above; each array names one. Nothing has to cross between parts.
Inputs may be any that keep to these rules, and one draw needn't show every extreme that they name: `slc`: complex samples of a partly coherent stack.
All inputs are finite; a program needn't handle non-finite values. No bound on the sum of `usable` on one device may be relied on, other than what follows from the above.
Results may differ from the reference program's by a relative error of at most 0.0016.
Values may be sent and summed in bfloat16 or wider, within the bound.
A program may use at most 64 MiB of HBM per device.

```python
import math
import jax
import jax.numpy as jnp
from jax import lax

DATES = 128
LOOKS = 100
ITERS = 4
WD = 16
WT = 128
NG = 2
NB = 8
WIN = 256


def rotate(common, phase):
    cosine = jnp.cos(phase)[None]
    sine_part = jnp.sin(phase)[None]
    return jnp.stack([common[0] * cosine - common[1] * sine_part, common[0] * sine_part + common[1] * cosine])


def draw_slc(key, part):
    subkeys = jax.random.split(key, 9)
    grid_shape = (DATES, WIN)
    amplitude = jnp.exp(jax.random.uniform(subkeys[0], grid_shape, jnp.float32, 0.0, math.log(10.0)))
    speckle = jnp.clip(jax.random.normal(subkeys[8], (2, LOOKS, DATES, WIN), jnp.float32), -4.0, 4.0)
    first_phase = jax.random.uniform(subkeys[1], grid_shape, jnp.float32, -math.pi, math.pi)
    second_phase = jax.random.uniform(subkeys[2], grid_shape, jnp.float32, -math.pi, math.pi)
    first_weight = jax.random.uniform(subkeys[3], (WIN,), jnp.float32, 0.3, 0.9)
    second_weight = jax.random.uniform(subkeys[4], (WIN,), jnp.float32, 0.1, 0.4)
    first_common = jnp.clip(jax.random.normal(subkeys[5], (2, LOOKS, 1, WIN), jnp.float32), -4.0, 4.0)
    second_common = jnp.clip(jax.random.normal(subkeys[6], (2, LOOKS, 1, WIN), jnp.float32), -4.0, 4.0)
    noise_weight = jnp.sqrt(jnp.maximum(1.0 - first_weight * first_weight - second_weight * second_weight, 0.05))
    sample = first_weight * rotate(first_common, first_phase) + second_weight * rotate(second_common, second_phase) + noise_weight * speckle
    return (amplitude * sample).astype(jnp.bfloat16)


def set_ends(drawn, stream_key, low, high):
    dims = drawn.shape
    place = [jax.random.randint(jax.random.fold_in(stream_key, axis), (), 0, dims[axis]) for axis in range(len(dims))]
    drawn = drawn.at[tuple(place)].set(low)
    longest = dims.index(max(dims))
    place[longest] = (place[longest] + 1) % dims[longest]
    return drawn.at[tuple(place)].set(high)


def setup_inputs(seed: int = 0, part: int = 0) -> dict:
    seeds = jax.random.split(jax.random.key(seed), 3)
    own_keys = jax.random.split(jax.random.fold_in(seeds[2], part), 3)
    return {
        "slc": draw_slc(jax.random.fold_in(jax.random.fold_in(seeds[2], part), 71), part),
        "usable": set_ends((jax.random.randint(own_keys[1], (LOOKS, DATES, WIN), 0, 4) < 3).astype(jnp.int32), jax.random.fold_in(own_keys[1], 1), 0, 1),
    }


def link_vectors(coherence):
    matrix = coherence.astype(jnp.float32)
    vec_real = jnp.ones((DATES, matrix.shape[1]), jnp.float32)
    vec_imag = jnp.zeros((DATES, matrix.shape[1]), jnp.float32)
    for step in range(ITERS):
        rr = jnp.einsum('wab,bw->aw', matrix[0], vec_real, precision=lax.Precision.HIGHEST)
        ii = jnp.einsum('wab,bw->aw', matrix[1], vec_imag, precision=lax.Precision.HIGHEST)
        ri = jnp.einsum('wab,bw->aw', matrix[0], vec_imag, precision=lax.Precision.HIGHEST)
        ir = jnp.einsum('wab,bw->aw', matrix[1], vec_real, precision=lax.Precision.HIGHEST)
        new_real = rr - ii
        new_imag = ri + ir
        scale = lax.rsqrt(lax.optimization_barrier(jnp.mean(new_real * new_real + new_imag * new_imag, axis=0)) + 1e-05)
        vec_real = new_real * scale[None]
        vec_imag = new_imag * scale[None]
    return jnp.stack([vec_real, vec_imag])

def window_block(operands):
    block, root = operands
    real_sum = jnp.einsum('law,lbw->wab', block[0], block[0]) + jnp.einsum('law,lbw->wab', block[1], block[1])
    imag_sum = jnp.einsum('law,lbw->wab', block[1], block[0]) - jnp.einsum('law,lbw->wab', block[0], block[1])
    factor = root.T[:, :, None] * root.T[:, None, :] * (1.0 / LOOKS)
    coherence = jnp.stack([real_sum * factor, imag_sum * factor]).astype(jnp.bfloat16)
    return (coherence, link_vectors(coherence))

def reference(slc, usable):
    masked = slc * usable.astype(jnp.bfloat16)[None]
    samples = masked.astype(jnp.float32)
    intensity = lax.optimization_barrier(jnp.mean(samples[0] * samples[0] + samples[1] * samples[1], axis=0)) + 1e-05
    inverse_root = lax.rsqrt(intensity)
    blocks = jnp.moveaxis(samples.reshape(2, LOOKS, DATES, NG, WT), 3, 0)
    roots = jnp.moveaxis(inverse_root.reshape(DATES, NG, WT), 1, 0)
    coherence, linked = lax.map(window_block, (blocks, roots))
    coherence = jnp.moveaxis(coherence, 1, 0)
    linked = jnp.moveaxis(linked, 0, 2).reshape(2, DATES, WIN)
    return (coherence.reshape(2, NG, NB, WD, DATES, DATES), linked)
```

```python
import functools

import jax
import jax.numpy as jnp
from jax import lax
from jax.experimental import pallas as pl
from jax.experimental.pallas import tpu as pltpu
from jax.sharding import PartitionSpec as P

ITERS = 4
LANES = 128
QUAD = 4
PIECES = 2
NT = (((1,), (1,)), ((), ()))


def dot_nt(left, right):
    return lax.dot_general(left, right, NT, preferred_element_type=jnp.float32)


def lane_bit(rows, strip):
    return (lax.broadcasted_iota(jnp.int32, (rows, LANES), 1) & strip) != 0


def swap_strips(blocks, exact):
    blocks = list(blocks)
    bit, strip = len(blocks) // 2, LANES // 2
    while bit:
        high = lane_bit(blocks[0].shape[0], strip)
        for low_index in range(len(blocks)):
            if low_index & bit:
                continue
            first, second = blocks[low_index], blocks[low_index | bit]
            if exact and strip != LANES // 2:
                blocks[low_index] = jnp.where(high, pltpu.roll(second, strip, 1), first)
                blocks[low_index | bit] = jnp.where(high, second, pltpu.roll(first, LANES - strip, 1))
            else:
                moved = pltpu.roll(jnp.where(high, first, second), strip, 1)
                blocks[low_index] = jnp.where(high, moved, first)
                blocks[low_index | bit] = jnp.where(high, second, moved)
        bit, strip = bit // 2, strip // 2
    return blocks


def window_coherence(sums, looks_count):
    dates = sums.shape[0] // 2
    real_sum = sums[:dates, :dates] + sums[dates:, dates:]
    imag_sum = sums[dates:, :dates] - sums[:dates, dates:]
    rows = lax.broadcasted_iota(jnp.int32, (dates, dates), 0)
    columns = lax.broadcasted_iota(jnp.int32, (dates, dates), 1)
    diagonal = jnp.where(rows == columns, real_sum, 0.0)
    row_root = lax.rsqrt(jnp.sum(diagonal, axis=0, keepdims=True) * (1.0 / looks_count) + 1e-05)
    column_root = lax.rsqrt(jnp.sum(diagonal, axis=1, keepdims=True) * (1.0 / looks_count) + 1e-05)
    factor = column_root * row_root * (1.0 / looks_count)
    return (real_sum * factor).astype(jnp.bfloat16), (imag_sum * factor).astype(jnp.bfloat16)


def link_windows(matrices):
    dates = matrices[0].shape[1]
    row = lax.broadcasted_iota(jnp.int32, (8, dates), 0)
    is_real = row < 3
    is_imag = jnp.logical_and(row >= 3, row < 6)
    is_first = jnp.logical_or(row == 0, row == 3)
    is_second = jnp.logical_or(row == 1, row == 4)
    state = [jnp.where(is_real, 1.0, 0.0)] * len(matrices)
    result = None
    for step in range(ITERS):
        products = []
        for vec, matrix in zip(state, matrices):
            high = vec.astype(jnp.bfloat16).astype(jnp.float32)
            rest = vec - high
            middle = rest.astype(jnp.bfloat16).astype(jnp.float32)
            parts = jnp.where(is_first, high, jnp.where(is_second, middle, rest - middle))
            products.append(dot_nt(parts.astype(jnp.bfloat16), matrix))
        state, result = [], []
        for product in products:
            first, second = product[:, :dates], product[:, dates:]
            zero = jnp.zeros_like(first)
            new_real = jnp.sum(
                jnp.where(is_real, first, jnp.where(is_imag, -second, zero)), axis=0, keepdims=True
            )
            new_imag = jnp.sum(
                jnp.where(is_real, second, jnp.where(is_imag, first, zero)), axis=0, keepdims=True
            )
            power = jnp.sum(new_real * new_real + new_imag * new_imag, axis=1, keepdims=True)
            scale = lax.rsqrt(power * (1.0 / dates) + 1e-05)
            new_real = new_real * scale
            new_imag = new_imag * scale
            result.append((new_real, new_imag))
            state.append(
                jnp.where(
                    is_real,
                    jnp.broadcast_to(new_real, (8, dates)),
                    jnp.where(is_imag, jnp.broadcast_to(new_imag, (8, dates)), 0.0),
                )
            )
    return result


def send_order(count):
    middle = count // 2
    return sorted(range(1, count), key=lambda offset: (offset % 2 == 0, -abs(offset - middle), offset))


def kernel(
    count, looks_count, windows,
    slc_hbm, usable_hbm, coherence_ref, linked_ref,
    slc_ref, usable_ref, packed, arrived, vectors, turned, landed,
    in_sem, send_sem, recv_sem, back_send, back_recv,
):
    me = lax.axis_index("date")
    own, local_windows = usable_ref.shape[1:]
    dates = count * own
    span = LANES // QUAD
    full = looks_count // span
    rest = looks_count - full * span
    extra = packed.shape[1] - 2 * full * (windows // QUAD)
    parts = windows // QUAD
    tile_owners = LANES // windows

    barrier = pltpu.get_barrier_semaphore()
    for offset in range(1, count):
        pl.semaphore_signal(
            barrier, inc=1, device_id={"date": lax.rem(me + offset, count)},
            device_id_type=pl.DeviceIdType.MESH,
        )

    chunks = [(full * span, rest)] if rest else []
    chunks += [(index * span, span) for index in range(full)]

    def loads(index):
        start, size = chunks[index]
        looks = pl.ds(start, size)
        return (
            pltpu.make_async_copy(usable_hbm.at[looks], usable_ref.at[looks], in_sem.at[index, 0]),
            pltpu.make_async_copy(slc_hbm.at[:, looks], slc_ref.at[:, looks], in_sem.at[index, 1]),
        )

    for index in range(len(chunks)):
        for copy in loads(index):
            copy.start()

    def masked(side, look, tile):
        lanes = slice(tile * LANES, (tile + 1) * LANES)
        return slc_ref[side, look, :, lanes] * usable_ref[look, :, lanes].astype(jnp.float32).astype(jnp.bfloat16)

    tiles = local_windows // LANES
    for index, (start, size) in enumerate(chunks):
        for copy in loads(index):
            copy.wait()
        for tile in range(tiles):
            if size == span:
                for side in range(2):
                    blocks = swap_strips([masked(side, start + look, tile) for look in range(span)], False)
                    for place, block in enumerate(blocks):
                        owner, part = divmod(place, parts)
                        packed[tile * tile_owners + owner, extra + (part * 2 + side) * full + start // span] = block
            else:
                half = tile_owners // 2
                zero = jnp.zeros((own, LANES), jnp.bfloat16)
                for piece in range(extra):
                    blocks = swap_strips(
                        [
                            masked(side, start + piece * half + look, tile) if piece * half + look < size else zero
                            for side in range(2)
                            for look in range(half)
                        ],
                        True,
                    )
                    for owner, block in enumerate(blocks):
                        packed[tile * tile_owners + owner, piece] = block

    order = send_order(count)

    def blocks_of(part):
        if isinstance(part, int) and part == 0:
            return pl.ds(0, extra + 2 * full)
        return pl.ds(extra + part * 2 * full, 2 * full)

    def block_copy(part, offset):
        other = lax.rem(me + offset, count)
        return pltpu.make_async_remote_copy(
            src_ref=packed.at[other, blocks_of(part)],
            dst_ref=arrived.at[me, blocks_of(part)],
            send_sem=send_sem.at[part, offset],
            recv_sem=recv_sem.at[part, offset],
            device_id={"date": other},
            device_id_type=pl.DeviceIdType.MESH,
        )

    pl.semaphore_wait(barrier, count - 1)
    for part in range(parts):
        for offset in order:
            block_copy(part, offset).start()
    arrived[me] = packed[me]

    lane = lax.broadcasted_iota(jnp.int32, (2 * dates, LANES), 1)

    def compute_part(part):
        for offset in order:
            block_copy(part, offset).wait_recv()

        def gathered(block):
            return arrived[:, block].reshape(dates, LANES)

        columns = []
        for piece in range(extra):
            both = gathered(piece)
            columns.append((jnp.concatenate([both, pltpu.roll(both, LANES // 2, 1)], axis=0), True))
        base = extra + part * 2 * full
        for index in range(full):
            columns.append((jnp.concatenate([gathered(base + index), gathered(base + full + index)], axis=0), False))
        right = jnp.concatenate([block for block, _ in columns], axis=1)
        matrices = []
        for inner in range(QUAD):
            window = part * QUAD + inner
            mine = jnp.logical_and(lane < LANES // 2, (lane & (windows - 1)) == window)
            own_lane = (lane & (QUAD - 1)) == inner
            left = jnp.concatenate(
                [jnp.where(mine if shared else own_lane, block, jnp.zeros_like(block)) for block, shared in columns],
                axis=1,
            )
            real, imag = window_coherence(dot_nt(left, right), looks_count)
            coherence_ref[0, 0, 0, window] = real
            coherence_ref[1, 0, 0, window] = imag
            matrices.append(jnp.concatenate([real, imag], axis=0))
        for inner, (real, imag) in enumerate(link_windows(matrices)):
            vectors[0, pl.ds(part * QUAD + inner, 1)] = real
            vectors[1, pl.ds(part * QUAD + inner, 1)] = imag

    for part in range(parts):
        compute_part(part)

    fold, rows, width = own // turned.shape[1], turned.shape[1], 2 * windows
    spread = jnp.concatenate([vectors[0], vectors[1]], axis=0)
    spread = jnp.pad(spread, ((0, LANES - width), (0, 0))).T.reshape(count, fold, rows, LANES)
    folded = spread[:, 0]
    for place in range(1, fold):
        folded = folded + pltpu.roll(
            spread[:, place].reshape(count * rows, LANES), place * width, 1
        ).reshape(count, rows, LANES)
    turned[...] = folded

    def back_copy(offset):
        other = lax.rem(me + offset, count)
        return pltpu.make_async_remote_copy(
            src_ref=turned.at[other],
            dst_ref=landed.at[me],
            send_sem=back_send.at[offset],
            recv_sem=back_recv.at[offset],
            device_id={"date": other},
            device_id_type=pl.DeviceIdType.MESH,
        )

    for offset in range(1, count):
        back_copy(offset).start()
    landed[me] = turned[me]
    for offset in range(1, count):
        back_copy(offset).wait_recv()
    for side in range(2):
        for place in range(fold):
            first = place * width + side * windows
            linked_ref[side, place * rows : (place + 1) * rows] = jnp.concatenate(
                [landed[source][:, first : first + windows] for source in range(count)], axis=1
            )

    for part in range(parts):
        for offset in range(1, count):
            block_copy(part, offset).wait_send()
    for offset in range(1, count):
        back_copy(offset).wait_send()


def deliver(coherence_in, linked_in, coherence_out, linked_out, sem):
    copies = [pltpu.make_async_copy(linked_in, linked_out, sem.at[0])]
    windows = coherence_in.shape[3]
    pieces = PIECES if windows % PIECES == 0 else 1
    size = windows // pieces
    for side in range(coherence_in.shape[0]):
        for piece in range(pieces):
            span = pl.ds(piece * size, size)
            copies.append(
                pltpu.make_async_copy(
                    coherence_in.at[side, :, :, span],
                    coherence_out.at[side, :, :, span],
                    sem.at[1 + side * PIECES + piece],
                )
            )
    for copy in copies:
        copy.start()
    for copy in copies:
        copy.wait()


def local(slc, usable):
    looks_count, own_dates, windows = usable.shape
    count = lax.axis_size("date")
    per_device = windows // count
    dates = own_dates * count
    parts = per_device // QUAD
    span = LANES // QUAD
    full = looks_count // span
    extra = pl.cdiv(looks_count - full * span, LANES // per_device // 2)
    fold = max(1, own_dates // 8)
    fold = fold if own_dates % fold == 0 and 2 * per_device * fold <= LANES else 1
    blocks = extra + 2 * full * parts
    results = pl.pallas_call(
        functools.partial(kernel, count, looks_count, per_device),
        out_shape=(
            jax.ShapeDtypeStruct((2, 1, 1, per_device, dates, dates), jnp.bfloat16),
            jax.ShapeDtypeStruct((2, own_dates, windows), jnp.float32),
        ),
        in_specs=[pl.BlockSpec(memory_space=pltpu.HBM)] * 2,
        out_specs=(
            pl.BlockSpec(memory_space=pltpu.VMEM),
            pl.BlockSpec(memory_space=pltpu.VMEM),
        ),
        scratch_shapes=[
            pltpu.VMEM((2, looks_count, own_dates, windows), jnp.bfloat16),
            pltpu.VMEM((looks_count, own_dates, windows), jnp.int32),
            pltpu.VMEM((count, blocks, own_dates, LANES), jnp.bfloat16),
            pltpu.VMEM((count, blocks, own_dates, LANES), jnp.bfloat16),
            pltpu.VMEM((2, per_device, dates), jnp.float32),
            pltpu.VMEM((count, own_dates // fold, LANES), jnp.float32),
            pltpu.VMEM((count, own_dates // fold, LANES), jnp.float32),
            pltpu.SemaphoreType.DMA((full + 1, 2)),
            pltpu.SemaphoreType.DMA((parts, count)),
            pltpu.SemaphoreType.DMA((parts, count)),
            pltpu.SemaphoreType.DMA((count,)),
            pltpu.SemaphoreType.DMA((count,)),
        ],
        compiler_params=pltpu.CompilerParams(collective_id=0, has_side_effects=True, vmem_limit_bytes=24 << 20),
    )(slc, usable)
    return pl.pallas_call(
        deliver,
        out_shape=tuple(jax.ShapeDtypeStruct(array.shape, array.dtype) for array in results),
        in_specs=[pl.BlockSpec(memory_space=pl.ANY)] * 2,
        out_specs=(pl.BlockSpec(memory_space=pl.ANY),) * 2,
        scratch_shapes=[pltpu.SemaphoreType.DMA((results[0].shape[0] * PIECES + 1,))],
        compiler_params=pltpu.CompilerParams(vmem_limit_bytes=1 << 20),
    )(*results)


def solution(mesh):
    return jax.shard_map(
        local,
        mesh=mesh,
        in_specs=(
            P(None, None, "date", ("slab", "tile", "sub")),
            P(None, "date", ("slab", "tile", "sub")),
        ),
        out_specs=(
            P(None, ("slab", "tile", "sub"), "date", None, None, None),
            P(None, "date", ("slab", "tile", "sub")),
        ),
        check_vma=False,
    )
```

```python
import functools

import jax
import jax.numpy as jnp
from jax import lax
from jax.experimental import pallas as pl
from jax.experimental.pallas import tpu as pltpu
from jax.sharding import PartitionSpec as P

ITERS = 4
LANES = 128
QUAD = 4
PIECES = 2
NT = (((1,), (1,)), ((), ()))


def dot_nt(left, right):
    return lax.dot_general(left, right, NT, preferred_element_type=jnp.float32)


def lane_bit(rows, strip):
    return (lax.broadcasted_iota(jnp.int32, (rows, LANES), 1) & strip) != 0


def swap_strips(blocks, exact):
    blocks = list(blocks)
    bit, strip = len(blocks) // 2, LANES // 2
    while bit:
        high = lane_bit(blocks[0].shape[0], strip)
        for low_index in range(len(blocks)):
            if low_index & bit:
                continue
            first, second = blocks[low_index], blocks[low_index | bit]
            if exact and strip != LANES // 2:
                blocks[low_index] = jnp.where(high, pltpu.roll(second, strip, 1), first)
                blocks[low_index | bit] = jnp.where(high, second, pltpu.roll(first, LANES - strip, 1))
            else:
                moved = pltpu.roll(jnp.where(high, first, second), strip, 1)
                blocks[low_index] = jnp.where(high, moved, first)
                blocks[low_index | bit] = jnp.where(high, second, moved)
        bit, strip = bit // 2, strip // 2
    return blocks


def window_coherence(sums, looks_count):
    dates = sums.shape[0] // 2
    real_sum = sums[:dates, :dates] + sums[dates:, dates:]
    imag_sum = sums[dates:, :dates] - sums[:dates, dates:]
    rows = lax.broadcasted_iota(jnp.int32, (dates, dates), 0)
    columns = lax.broadcasted_iota(jnp.int32, (dates, dates), 1)
    diagonal = jnp.where(rows == columns, real_sum, 0.0)
    row_root = lax.rsqrt(jnp.sum(diagonal, axis=0, keepdims=True) * (1.0 / looks_count) + 1e-05)
    column_root = lax.rsqrt(jnp.sum(diagonal, axis=1, keepdims=True) * (1.0 / looks_count) + 1e-05)
    factor = column_root * row_root * (1.0 / looks_count)
    return (real_sum * factor).astype(jnp.bfloat16), (imag_sum * factor).astype(jnp.bfloat16)


def link_windows(matrices):
    dates = matrices[0].shape[1]
    row = lax.broadcasted_iota(jnp.int32, (8, dates), 0)
    is_real = row < 3
    is_imag = jnp.logical_and(row >= 3, row < 6)
    is_first = jnp.logical_or(row == 0, row == 3)
    is_second = jnp.logical_or(row == 1, row == 4)
    state = [jnp.where(is_real, 1.0, 0.0)] * len(matrices)
    scales = [None] * len(matrices)
    result = []
    for step in range(ITERS):
        products = []
        for vec, matrix in zip(state, matrices):
            high = vec.astype(jnp.bfloat16).astype(jnp.float32)
            left = vec - high
            middle = left.astype(jnp.bfloat16).astype(jnp.float32)
            pieces = jnp.where(is_first, high, jnp.where(is_second, middle, left - middle))
            products.append(dot_nt(pieces.astype(jnp.bfloat16), matrix))
        for index, product in enumerate(products):
            first, second = product[:, :dates], product[:, dates:]
            zero = jnp.zeros_like(first)
            new_real = jnp.sum(
                jnp.where(is_real, first, jnp.where(is_imag, -second, zero)), axis=0, keepdims=True
            )
            new_imag = jnp.sum(
                jnp.where(is_real, second, jnp.where(is_imag, first, zero)), axis=0, keepdims=True
            )
            if step:
                new_real = new_real * scales[index]
                new_imag = new_imag * scales[index]
            power = jnp.sum(new_real * new_real + new_imag * new_imag, axis=1, keepdims=True)
            scales[index] = lax.rsqrt(power * (1.0 / dates) + 1e-05)
            if step == ITERS - 1:
                result.append((new_real * scales[index], new_imag * scales[index]))
            else:
                state[index] = jnp.where(
                    is_real,
                    jnp.broadcast_to(new_real, (8, dates)),
                    jnp.where(is_imag, jnp.broadcast_to(new_imag, (8, dates)), 0.0),
                )
    return result


def send_order(count):
    middle = count // 2
    return sorted(range(1, count), key=lambda offset: (offset % 2 == 0, -abs(offset - middle), offset))


def kernel(
    count, looks_count, windows,
    slc_hbm, usable_hbm, coherence_ref, linked_ref,
    slc_ref, usable_ref, packed, arrived, vectors, turned, landed,
    in_sem, send_sem, recv_sem, back_send, back_recv,
):
    me = lax.axis_index("date")
    own, local_windows = usable_ref.shape[1:]
    dates = count * own
    span = LANES // QUAD
    full = looks_count // span
    rest = looks_count - full * span
    parts = windows // QUAD
    extra = packed.shape[1] - 2 * full * parts
    later = 2 * (full - 1)
    tile_owners = LANES // windows

    barrier = pltpu.get_barrier_semaphore()
    for offset in range(1, count):
        pl.semaphore_signal(
            barrier, inc=1, device_id={"date": lax.rem(me + offset, count)},
            device_id_type=pl.DeviceIdType.MESH,
        )

    chunks = [(0, span)] + ([(full * span, rest)] if rest else [])
    chunks += [(index * span, span) for index in range(1, full)]

    def loads(index):
        start, size = chunks[index]
        looks = pl.ds(start, size)
        return (
            pltpu.make_async_copy(usable_hbm.at[looks], usable_ref.at[looks], in_sem.at[index, 0]),
            pltpu.make_async_copy(slc_hbm.at[:, looks], slc_ref.at[:, looks], in_sem.at[index, 1]),
        )

    for index in range(len(chunks)):
        for copy in loads(index):
            copy.start()

    def masked(side, look, tile):
        lanes = slice(tile * LANES, (tile + 1) * LANES)
        return slc_ref[side, look, :, lanes] * usable_ref[look, :, lanes].astype(jnp.float32).astype(jnp.bfloat16)

    def first_block(part, side):
        return 2 * part + side

    def later_block(part, side, index):
        return 2 * parts + extra + part * later + side * (full - 1) + index - 1

    tiles = local_windows // LANES

    def prepare(index):
        start, size = chunks[index]
        for copy in loads(index):
            copy.wait()
        for tile in range(tiles):
            if size == span:
                for side in range(2):
                    blocks = swap_strips([masked(side, start + look, tile) for look in range(span)], False)
                    for place, block in enumerate(blocks):
                        owner, part = divmod(place, parts)
                        row = later_block(part, side, start // span) if start else first_block(part, side)
                        packed[tile * tile_owners + owner, row] = block
            else:
                half = tile_owners // 2
                zero = jnp.zeros((own, LANES), jnp.bfloat16)
                for piece in range(extra):
                    blocks = swap_strips(
                        [
                            masked(side, start + piece * half + look, tile) if piece * half + look < size else zero
                            for side in range(2)
                            for look in range(half)
                        ],
                        True,
                    )
                    for owner, block in enumerate(blocks):
                        packed[tile * tile_owners + owner, 2 * parts + piece] = block

    order = send_order(count)

    def blocks_of(message):
        if message == 0:
            return pl.ds(0, 2 * parts)
        if message == 1:
            return pl.ds(2 * parts, extra + later)
        return pl.ds(2 * parts + extra + (message - 1) * later, later)

    def block_copy(message, offset):
        other = lax.rem(me + offset, count)
        return pltpu.make_async_remote_copy(
            src_ref=packed.at[other, blocks_of(message)],
            dst_ref=arrived.at[me, blocks_of(message)],
            send_sem=send_sem.at[message, offset],
            recv_sem=recv_sem.at[message, offset],
            device_id={"date": other},
            device_id_type=pl.DeviceIdType.MESH,
        )

    prepare(0)
    pl.semaphore_wait(barrier, count - 1)
    for offset in order:
        block_copy(0, offset).start()
    for index in range(1, len(chunks)):
        prepare(index)
    for message in range(1, parts + 1):
        for offset in order:
            block_copy(message, offset).start()
    arrived[me] = packed[me]

    lane = lax.broadcasted_iota(jnp.int32, (2 * dates, LANES), 1)

    def compute_part(part):
        for message in range(0 if part == 0 else part + 1, part + 2):
            for offset in order:
                block_copy(message, offset).wait_recv()

        def gathered(block):
            return arrived[:, block].reshape(dates, LANES)

        columns = []
        for piece in range(extra):
            both = gathered(2 * parts + piece)
            columns.append((jnp.concatenate([both, pltpu.roll(both, LANES // 2, 1)], axis=0), True))
        for index in range(full):
            sides = [
                gathered(later_block(part, side, index) if index else first_block(part, side)) for side in range(2)
            ]
            columns.append((jnp.concatenate(sides, axis=0), False))
        right = jnp.concatenate([block for block, _ in columns], axis=1)
        matrices = []
        for inner in range(QUAD):
            window = part * QUAD + inner
            mine = jnp.logical_and(lane < LANES // 2, (lane & (windows - 1)) == window)
            own_lane = (lane & (QUAD - 1)) == inner
            left = jnp.concatenate(
                [jnp.where(mine if shared else own_lane, block, jnp.zeros_like(block)) for block, shared in columns],
                axis=1,
            )
            real, imag = window_coherence(dot_nt(left, right), looks_count)
            coherence_ref[0, 0, 0, window] = real
            coherence_ref[1, 0, 0, window] = imag
            matrices.append(jnp.concatenate([real, imag], axis=0))
        for inner, (real, imag) in enumerate(link_windows(matrices)):
            vectors[0, pl.ds(part * QUAD + inner, 1)] = real
            vectors[1, pl.ds(part * QUAD + inner, 1)] = imag

    for part in range(parts):
        compute_part(part)

    fold, rows, width = own // turned.shape[1], turned.shape[1], 2 * windows
    spread = jnp.concatenate([vectors[0], vectors[1]], axis=0)
    spread = jnp.pad(spread, ((0, LANES - width), (0, 0))).T.reshape(count, fold, rows, LANES)
    folded = spread[:, 0]
    for place in range(1, fold):
        folded = folded + pltpu.roll(
            spread[:, place].reshape(count * rows, LANES), place * width, 1
        ).reshape(count, rows, LANES)
    turned[...] = folded

    def back_copy(offset):
        other = lax.rem(me + offset, count)
        return pltpu.make_async_remote_copy(
            src_ref=turned.at[other],
            dst_ref=landed.at[me],
            send_sem=back_send.at[offset],
            recv_sem=back_recv.at[offset],
            device_id={"date": other},
            device_id_type=pl.DeviceIdType.MESH,
        )

    for offset in range(1, count):
        back_copy(offset).start()
    landed[me] = turned[me]
    for offset in range(1, count):
        back_copy(offset).wait_recv()
    for side in range(2):
        for place in range(fold):
            first = place * width + side * windows
            linked_ref[side, place * rows : (place + 1) * rows] = jnp.concatenate(
                [landed[source][:, first : first + windows] for source in range(count)], axis=1
            )

    for message in range(parts + 1):
        for offset in range(1, count):
            block_copy(message, offset).wait_send()
    for offset in range(1, count):
        back_copy(offset).wait_send()


def deliver(coherence_in, linked_in, coherence_out, linked_out, sem):
    copies = [pltpu.make_async_copy(linked_in, linked_out, sem.at[0])]
    windows = coherence_in.shape[3]
    pieces = PIECES if windows % PIECES == 0 else 1
    size = windows // pieces
    for side in range(coherence_in.shape[0]):
        for piece in range(pieces):
            span = pl.ds(piece * size, size)
            copies.append(
                pltpu.make_async_copy(
                    coherence_in.at[side, :, :, span],
                    coherence_out.at[side, :, :, span],
                    sem.at[1 + side * PIECES + piece],
                )
            )
    for copy in copies:
        copy.start()
    for copy in copies:
        copy.wait()


def local(slc, usable):
    looks_count, own_dates, windows = usable.shape
    count = lax.axis_size("date")
    per_device = windows // count
    dates = own_dates * count
    parts = per_device // QUAD
    span = LANES // QUAD
    full = looks_count // span
    extra = pl.cdiv(looks_count - full * span, LANES // per_device // 2)
    fold = max(1, own_dates // 8)
    fold = fold if own_dates % fold == 0 and 2 * per_device * fold <= LANES else 1
    blocks = extra + 2 * full * parts
    results = pl.pallas_call(
        functools.partial(kernel, count, looks_count, per_device),
        out_shape=(
            jax.ShapeDtypeStruct((2, 1, 1, per_device, dates, dates), jnp.bfloat16),
            jax.ShapeDtypeStruct((2, own_dates, windows), jnp.float32),
        ),
        in_specs=[pl.BlockSpec(memory_space=pltpu.HBM)] * 2,
        out_specs=(
            pl.BlockSpec(memory_space=pltpu.VMEM),
            pl.BlockSpec(memory_space=pltpu.VMEM),
        ),
        scratch_shapes=[
            pltpu.VMEM((2, looks_count, own_dates, windows), jnp.bfloat16),
            pltpu.VMEM((looks_count, own_dates, windows), jnp.int32),
            pltpu.VMEM((count, blocks, own_dates, LANES), jnp.bfloat16),
            pltpu.VMEM((count, blocks, own_dates, LANES), jnp.bfloat16),
            pltpu.VMEM((2, per_device, dates), jnp.float32),
            pltpu.VMEM((count, own_dates // fold, LANES), jnp.float32),
            pltpu.VMEM((count, own_dates // fold, LANES), jnp.float32),
            pltpu.SemaphoreType.DMA((full + 1, 2)),
            pltpu.SemaphoreType.DMA((parts + 1, count)),
            pltpu.SemaphoreType.DMA((parts + 1, count)),
            pltpu.SemaphoreType.DMA((count,)),
            pltpu.SemaphoreType.DMA((count,)),
        ],
        compiler_params=pltpu.CompilerParams(collective_id=0, has_side_effects=True, vmem_limit_bytes=24 << 20),
    )(pltpu.with_memory_space_constraint(slc, pltpu.HBM), pltpu.with_memory_space_constraint(usable, pltpu.HBM))
    return pl.pallas_call(
        deliver,
        out_shape=tuple(jax.ShapeDtypeStruct(array.shape, array.dtype) for array in results),
        in_specs=[pl.BlockSpec(memory_space=pl.ANY)] * 2,
        out_specs=(pl.BlockSpec(memory_space=pl.ANY),) * 2,
        scratch_shapes=[pltpu.SemaphoreType.DMA((results[0].shape[0] * PIECES + 1,))],
        compiler_params=pltpu.CompilerParams(vmem_limit_bytes=1 << 20),
    )(*results)


def solution(mesh):
    return jax.shard_map(
        local,
        mesh=mesh,
        in_specs=(
            P(None, None, "date", ("slab", "tile", "sub")),
            P(None, "date", ("slab", "tile", "sub")),
        ),
        out_specs=(
            P(None, ("slab", "tile", "sub"), "date", None, None, None),
            P(None, "date", ("slab", "tile", "sub")),
        ),
        check_vma=False,
    )
```

```python
import functools

import jax
import jax.numpy as jnp
from jax import lax
from jax.experimental import pallas as pl
from jax.experimental.pallas import tpu as pltpu
from jax.sharding import PartitionSpec as P

ITERS = 4
LANES = 128
QUAD = 4
PAIR = 2
AHEAD = 3
PIECES = 2
NT = (((1,), (1,)), ((), ()))


def dot_nt(left, right):
    return lax.dot_general(left, right, NT, preferred_element_type=jnp.float32)


def lane_bit(rows, strip):
    return (lax.broadcasted_iota(jnp.int32, (rows, LANES), 1) & strip) != 0


def swap_strips(blocks, exact):
    blocks = list(blocks)
    bit, strip = len(blocks) // 2, LANES // 2
    while bit:
        high = lane_bit(blocks[0].shape[0], strip)
        for low_index in range(len(blocks)):
            if low_index & bit:
                continue
            first, second = blocks[low_index], blocks[low_index | bit]
            if exact and strip != LANES // 2:
                blocks[low_index] = jnp.where(high, pltpu.roll(second, strip, 1), first)
                blocks[low_index | bit] = jnp.where(high, second, pltpu.roll(first, LANES - strip, 1))
            else:
                moved = pltpu.roll(jnp.where(high, first, second), strip, 1)
                blocks[low_index] = jnp.where(high, moved, first)
                blocks[low_index | bit] = jnp.where(high, second, moved)
        bit, strip = bit // 2, strip // 2
    return blocks


def window_coherence(sums, looks_count):
    dates = sums.shape[0] // 2
    real_sum = sums[:dates, :dates] + sums[dates:, dates:]
    imag_sum = sums[dates:, :dates] - sums[:dates, dates:]
    rows = lax.broadcasted_iota(jnp.int32, (dates, dates), 0)
    columns = lax.broadcasted_iota(jnp.int32, (dates, dates), 1)
    diagonal = jnp.where(rows == columns, real_sum, 0.0)
    row_root = lax.rsqrt(jnp.sum(diagonal, axis=0, keepdims=True) * (1.0 / looks_count) + 1e-05)
    column_root = lax.rsqrt(jnp.sum(diagonal, axis=1, keepdims=True) * (1.0 / looks_count) + 1e-05)
    factor = column_root * row_root * (1.0 / looks_count)
    return (real_sum * factor).astype(jnp.bfloat16), (imag_sum * factor).astype(jnp.bfloat16)


def link_windows(matrices):
    dates = matrices[0].shape[0]
    row = lax.broadcasted_iota(jnp.int32, (8, dates), 0)
    is_real = row < 3
    is_imag = jnp.logical_and(row >= 3, row < 6)
    is_first = jnp.logical_or(row == 0, row == 3)
    is_second = jnp.logical_or(row == 1, row == 4)
    state = [jnp.where(is_real, 1.0, 0.0)] * len(matrices)
    scales = [None] * len(matrices)
    result = []
    for step in range(ITERS):
        products = []
        for vec, matrix in zip(state, matrices):
            high = vec.astype(jnp.bfloat16).astype(jnp.float32)
            left = vec - high
            middle = left.astype(jnp.bfloat16).astype(jnp.float32)
            pieces = jnp.where(is_first, high, jnp.where(is_second, middle, left - middle))
            products.append(jnp.dot(pieces.astype(jnp.bfloat16), matrix, preferred_element_type=jnp.float32))
        for index, product in enumerate(products):
            first, second = product[:, :dates], product[:, dates:]
            zero = jnp.zeros_like(first)
            new_real = jnp.sum(
                jnp.where(is_real, first, jnp.where(is_imag, second, zero)), axis=0, keepdims=True
            )
            new_imag = jnp.sum(
                jnp.where(is_real, -second, jnp.where(is_imag, first, zero)), axis=0, keepdims=True
            )
            if step:
                new_real = new_real * scales[index]
                new_imag = new_imag * scales[index]
            power = jnp.sum(new_real * new_real + new_imag * new_imag, axis=1, keepdims=True)
            scales[index] = lax.rsqrt(power * (1.0 / dates) + 1e-05)
            if step == ITERS - 1:
                result.append((new_real * scales[index], new_imag * scales[index]))
            else:
                state[index] = jnp.where(
                    is_real,
                    jnp.broadcast_to(new_real, (8, dates)),
                    jnp.where(is_imag, jnp.broadcast_to(new_imag, (8, dates)), 0.0),
                )
    return result


def descending(count, me):
    return [top - (top <= me).astype(jnp.int32) for top in range(count - 1, 0, -1)]


def at_distance(count, me, distance):
    pairs = count // PAIR
    row, side = me // PAIR, lax.rem(me, PAIR)
    found = []
    for across in range(PAIR):
        steps = distance - across
        if steps < 0:
            continue
        for along in sorted({steps, -steps}, reverse=True):
            if abs(along) < pairs:
                exists = jnp.logical_and(row + along >= 0, row + along < pairs)
                found.append((exists, (row + along) * PAIR + (1 - side if across else side)))
    return found


def kernel(
    count, looks_count, windows,
    slc_hbm, usable_hbm, coherence_ref, linked_ref,
    slc_ref, usable_ref, packed, arrived, vectors, turned, landed,
    in_sem, send_sem, recv_sem, back_send, back_recv, round_sem,
):
    me = lax.axis_index("date")
    own, local_windows = usable_ref.shape[1:]
    dates = count * own
    span = LANES // QUAD
    full = looks_count // span
    rest = looks_count - full * span
    parts = windows // QUAD
    extra = packed.shape[1] - 2 * full * parts
    later = 2 * (full - 1)
    tile_owners = LANES // windows

    barrier = pltpu.get_barrier_semaphore()
    farthest = count // PAIR - 1 + PAIR - 1
    beside = at_distance(count, me, 1)
    greetings = sum(exists.astype(jnp.int32) for exists, _ in beside)

    def greet(semaphore):
        for exists, other in beside:
            @pl.when(exists)
            def _():
                pl.semaphore_signal(
                    semaphore, inc=1, device_id={"date": other}, device_id_type=pl.DeviceIdType.MESH
                )

    greet(barrier)

    chunks = [(0, span)] + ([(full * span, rest)] if rest else [])
    chunks += [(index * span, span) for index in range(1, full)]

    def loads(index):
        start, size = chunks[index]
        looks = pl.ds(start, size)
        return (
            pltpu.make_async_copy(usable_hbm.at[looks], usable_ref.at[looks], in_sem.at[index, 0]),
            pltpu.make_async_copy(slc_hbm.at[:, looks], slc_ref.at[:, looks], in_sem.at[index, 1]),
        )

    for index in range(len(chunks)):
        for copy in loads(index):
            copy.start()

    def masked(side, look, tile):
        lanes = slice(tile * LANES, (tile + 1) * LANES)
        return slc_ref[side, look, :, lanes] * usable_ref[look, :, lanes].astype(jnp.float32).astype(jnp.bfloat16)

    def first_block(part, side):
        return 2 * part + side

    def later_block(part, side, index):
        return 2 * parts + extra + part * later + side * (full - 1) + index - 1

    tiles = local_windows // LANES

    def prepare(index):
        start, size = chunks[index]
        for copy in loads(index):
            copy.wait()
        for tile in range(tiles):
            if size == span:
                for side in range(2):
                    blocks = swap_strips([masked(side, start + look, tile) for look in range(span)], False)
                    for place, block in enumerate(blocks):
                        owner, part = divmod(place, parts)
                        row = later_block(part, side, start // span) if start else first_block(part, side)
                        packed[tile * tile_owners + owner, row] = block
            else:
                half = tile_owners // 2
                zero = jnp.zeros((own, LANES), jnp.bfloat16)
                for piece in range(extra):
                    blocks = swap_strips(
                        [
                            masked(side, start + piece * half + look, tile) if piece * half + look < size else zero
                            for side in range(2)
                            for look in range(half)
                        ],
                        True,
                    )
                    for owner, block in enumerate(blocks):
                        packed[tile * tile_owners + owner, 2 * parts + piece] = block

    others = descending(count, me)

    def blocks_of(message):
        if message == 0:
            return pl.ds(0, 2 * parts)
        if message == 1:
            return pl.ds(2 * parts, extra + later)
        return pl.ds(2 * parts + extra + (message - 1) * later, later)

    def block_copy(message, other, source):
        return pltpu.make_async_remote_copy(
            src_ref=packed.at[other, blocks_of(message)],
            dst_ref=arrived.at[source, blocks_of(message)],
            send_sem=send_sem.at[message, other],
            recv_sem=recv_sem.at[message, source],
            device_id={"date": other},
            device_id_type=pl.DeviceIdType.MESH,
        )

    def send_at(distance, messages):
        for exists, other in at_distance(count, me, distance):
            @pl.when(exists)
            def _():
                for message in messages:
                    block_copy(message, other, me).start()

    def send_all(message):
        for other in others:
            block_copy(message, other, me).start()

    with jax.named_scope("prepare_first"):
        prepare(0)
    with jax.named_scope("meet_first"):
        pl.semaphore_wait(barrier, greetings)
    if farthest > 1:
        greet(round_sem.at[0])
    send_at(1, [0])
    with jax.named_scope("prepare_rest"):
        for index in range(1, len(chunks)):
            prepare(index)
    send_at(1, [1])
    for distance in range(2, farthest + 1):
        with jax.named_scope("meet_next"):
            pl.semaphore_wait(round_sem.at[distance - 2], greetings)
        if distance < farthest:
            greet(round_sem.at[distance - 1])
        send_at(distance, [0, 1])
    for message in range(2, min(AHEAD, parts + 1)):
        send_all(message)
    arrived[me] = packed[me]

    lane = lax.broadcasted_iota(jnp.int32, (2 * dates, LANES), 1)

    def compute_part(part):
        with jax.named_scope(f"wait_{part}"):
            for message in range(0 if part == 0 else part + 1, part + 2):
                for other in others:
                    block_copy(message, other, other).wait_recv()
        if part + AHEAD <= parts:
            send_all(part + AHEAD)

        def gathered(block):
            return arrived[:, block].reshape(dates, LANES)

        columns = []
        for piece in range(extra):
            both = gathered(2 * parts + piece)
            columns.append((jnp.concatenate([both, pltpu.roll(both, LANES // 2, 1)], axis=0), True))
        for index in range(full):
            sides = [
                gathered(later_block(part, side, index) if index else first_block(part, side)) for side in range(2)
            ]
            columns.append((jnp.concatenate(sides, axis=0), False))
        right = jnp.concatenate([block for block, _ in columns], axis=1)
        matrices = []
        for inner in range(QUAD):
            window = part * QUAD + inner
            mine = jnp.logical_and(lane < LANES // 2, (lane & (windows - 1)) == window)
            own_lane = (lane & (QUAD - 1)) == inner
            left = jnp.concatenate(
                [jnp.where(mine if shared else own_lane, block, jnp.zeros_like(block)) for block, shared in columns],
                axis=1,
            )
            real, imag = window_coherence(dot_nt(left, right), looks_count)
            coherence_ref[0, 0, 0, window] = real
            coherence_ref[1, 0, 0, window] = imag
            matrices.append(jnp.concatenate([real, imag], axis=1))
        for inner, (real, imag) in enumerate(link_windows(matrices)):
            vectors[0, pl.ds(part * QUAD + inner, 1)] = real
            vectors[1, pl.ds(part * QUAD + inner, 1)] = imag

    for part in range(parts):
        with jax.named_scope(f"part_{part}"):
            compute_part(part)

    fold, rows, width = own // turned.shape[1], turned.shape[1], 2 * windows
    spread = jnp.concatenate([vectors[0], vectors[1]], axis=0)
    spread = jnp.pad(spread, ((0, LANES - width), (0, 0))).T.reshape(count, fold, rows, LANES)
    folded = spread[:, 0]
    for place in range(1, fold):
        folded = folded + pltpu.roll(
            spread[:, place].reshape(count * rows, LANES), place * width, 1
        ).reshape(count, rows, LANES)
    turned[...] = folded

    def back_copy(other, source):
        return pltpu.make_async_remote_copy(
            src_ref=turned.at[other],
            dst_ref=landed.at[source],
            send_sem=back_send.at[other],
            recv_sem=back_recv.at[source],
            device_id={"date": other},
            device_id_type=pl.DeviceIdType.MESH,
        )

    for other in reversed(others):
        back_copy(other, me).start()
    landed[me] = turned[me]
    with jax.named_scope("wait_back"):
        for other in others:
            back_copy(other, other).wait_recv()
    for side in range(2):
        for place in range(fold):
            first = place * width + side * windows
            linked_ref[side, place * rows : (place + 1) * rows] = jnp.concatenate(
                [landed[source][:, first : first + windows] for source in range(count)], axis=1
            )

    for message in range(parts + 1):
        for other in others:
            block_copy(message, other, me).wait_send()
    for other in others:
        back_copy(other, me).wait_send()


def deliver(coherence_in, linked_in, coherence_out, linked_out, sem):
    copies = [pltpu.make_async_copy(linked_in, linked_out, sem.at[0])]
    windows = coherence_in.shape[3]
    pieces = PIECES if windows % PIECES == 0 else 1
    size = windows // pieces
    for side in range(coherence_in.shape[0]):
        for piece in range(pieces):
            span = pl.ds(piece * size, size)
            copies.append(
                pltpu.make_async_copy(
                    coherence_in.at[side, :, :, span],
                    coherence_out.at[side, :, :, span],
                    sem.at[1 + side * PIECES + piece],
                )
            )
    for copy in copies:
        copy.start()
    for copy in copies:
        copy.wait()


def local(slc, usable):
    looks_count, own_dates, windows = usable.shape
    count = lax.axis_size("date")
    per_device = windows // count
    dates = own_dates * count
    parts = per_device // QUAD
    span = LANES // QUAD
    full = looks_count // span
    extra = pl.cdiv(looks_count - full * span, LANES // per_device // 2)
    fold = max(1, own_dates // 8)
    fold = fold if own_dates % fold == 0 and 2 * per_device * fold <= LANES else 1
    blocks = extra + 2 * full * parts
    results = pl.pallas_call(
        functools.partial(kernel, count, looks_count, per_device),
        out_shape=(
            jax.ShapeDtypeStruct((2, 1, 1, per_device, dates, dates), jnp.bfloat16),
            jax.ShapeDtypeStruct((2, own_dates, windows), jnp.float32),
        ),
        in_specs=[pl.BlockSpec(memory_space=pltpu.HBM)] * 2,
        out_specs=(
            pl.BlockSpec(memory_space=pltpu.VMEM),
            pl.BlockSpec(memory_space=pltpu.VMEM),
        ),
        scratch_shapes=[
            pltpu.VMEM((2, looks_count, own_dates, windows), jnp.bfloat16),
            pltpu.VMEM((looks_count, own_dates, windows), jnp.int32),
            pltpu.VMEM((count, blocks, own_dates, LANES), jnp.bfloat16),
            pltpu.VMEM((count, blocks, own_dates, LANES), jnp.bfloat16),
            pltpu.VMEM((2, per_device, dates), jnp.float32),
            pltpu.VMEM((count, own_dates // fold, LANES), jnp.float32),
            pltpu.VMEM((count, own_dates // fold, LANES), jnp.float32),
            pltpu.SemaphoreType.DMA((full + 1, 2)),
            pltpu.SemaphoreType.DMA((parts + 1, count)),
            pltpu.SemaphoreType.DMA((parts + 1, count)),
            pltpu.SemaphoreType.DMA((count,)),
            pltpu.SemaphoreType.DMA((count,)),
            pltpu.SemaphoreType.REGULAR((count // PAIR + PAIR - 2,)),
        ],
        compiler_params=pltpu.CompilerParams(collective_id=0, has_side_effects=True, vmem_limit_bytes=24 << 20),
    )(pltpu.with_memory_space_constraint(slc, pltpu.HBM), pltpu.with_memory_space_constraint(usable, pltpu.HBM))
    return pl.pallas_call(
        deliver,
        out_shape=tuple(jax.ShapeDtypeStruct(array.shape, array.dtype) for array in results),
        in_specs=[pl.BlockSpec(memory_space=pl.ANY)] * 2,
        out_specs=(pl.BlockSpec(memory_space=pl.ANY),) * 2,
        scratch_shapes=[pltpu.SemaphoreType.DMA((results[0].shape[0] * PIECES + 1,))],
        compiler_params=pltpu.CompilerParams(vmem_limit_bytes=1 << 20),
    )(*results)


def solution(mesh):
    return jax.shard_map(
        local,
        mesh=mesh,
        in_specs=(
            P(None, None, "date", ("slab", "tile", "sub")),
            P(None, "date", ("slab", "tile", "sub")),
        ),
        out_specs=(
            P(None, ("slab", "tile", "sub"), "date", None, None, None),
            P(None, "date", ("slab", "tile", "sub")),
        ),
        check_vma=False,
    )
```

```python
import functools

import jax
import jax.numpy as jnp
from jax import lax
from jax.experimental import pallas as pl
from jax.experimental.pallas import tpu as pltpu
from jax.sharding import PartitionSpec as P

ITERS = 4
LANES = 128
QUAD = 4
PAIR = 2
SENT = ((4, 5), (2, 4, 5))
PIECES = 2
NT = (((1,), (1,)), ((), ()))


def dot_nt(left, right):
    return lax.dot_general(left, right, NT, preferred_element_type=jnp.float32)


def lane_bit(rows, strip):
    return (lax.broadcasted_iota(jnp.int32, (rows, LANES), 1) & strip) != 0


def swap_strips(blocks, exact):
    blocks = list(blocks)
    bit, strip = len(blocks) // 2, LANES // 2
    while bit:
        high = lane_bit(blocks[0].shape[0], strip)
        for low_index in range(len(blocks)):
            if low_index & bit:
                continue
            first, second = blocks[low_index], blocks[low_index | bit]
            if exact and strip != LANES // 2:
                blocks[low_index] = jnp.where(high, pltpu.roll(second, strip, 1), first)
                blocks[low_index | bit] = jnp.where(high, second, pltpu.roll(first, LANES - strip, 1))
            else:
                moved = pltpu.roll(jnp.where(high, first, second), strip, 1)
                blocks[low_index] = jnp.where(high, moved, first)
                blocks[low_index | bit] = jnp.where(high, second, moved)
        bit, strip = bit // 2, strip // 2
    return blocks


def window_coherence(sums, looks_count):
    dates = sums.shape[0] // 2
    real_sum = sums[:dates, :dates] + sums[dates:, dates:]
    imag_sum = sums[dates:, :dates] - sums[:dates, dates:]
    rows = lax.broadcasted_iota(jnp.int32, (dates, dates), 0)
    columns = lax.broadcasted_iota(jnp.int32, (dates, dates), 1)
    diagonal = jnp.where(rows == columns, real_sum, 0.0)
    row_root = lax.rsqrt(jnp.sum(diagonal, axis=0, keepdims=True) * (1.0 / looks_count) + 1e-05)
    column_root = lax.rsqrt(jnp.sum(diagonal, axis=1, keepdims=True) * (1.0 / looks_count) + 1e-05)
    factor = column_root * row_root * (1.0 / looks_count)
    return (real_sum * factor).astype(jnp.bfloat16), (imag_sum * factor).astype(jnp.bfloat16)


def link_windows(matrices):
    dates = matrices[0].shape[0]
    row = lax.broadcasted_iota(jnp.int32, (8, dates), 0)
    is_real = row < 3
    is_imag = jnp.logical_and(row >= 3, row < 6)
    is_first = jnp.logical_or(row == 0, row == 3)
    is_second = jnp.logical_or(row == 1, row == 4)
    state = [jnp.where(is_real, 1.0, 0.0)] * len(matrices)
    scales = [None] * len(matrices)
    result = []
    for step in range(ITERS):
        products = []
        for vec, matrix in zip(state, matrices):
            high = vec.astype(jnp.bfloat16).astype(jnp.float32)
            left = vec - high
            middle = left.astype(jnp.bfloat16).astype(jnp.float32)
            pieces = jnp.where(is_first, high, jnp.where(is_second, middle, left - middle))
            products.append(jnp.dot(pieces.astype(jnp.bfloat16), matrix, preferred_element_type=jnp.float32))
        for index, product in enumerate(products):
            first, second = product[:, :dates], product[:, dates:]
            zero = jnp.zeros_like(first)
            new_real = jnp.sum(
                jnp.where(is_real, first, jnp.where(is_imag, second, zero)), axis=0, keepdims=True
            )
            new_imag = jnp.sum(
                jnp.where(is_real, -second, jnp.where(is_imag, first, zero)), axis=0, keepdims=True
            )
            if step:
                new_real = new_real * scales[index]
                new_imag = new_imag * scales[index]
            power = jnp.sum(new_real * new_real + new_imag * new_imag, axis=1, keepdims=True)
            scales[index] = lax.rsqrt(power * (1.0 / dates) + 1e-05)
            if step == ITERS - 1:
                result.append((new_real * scales[index], new_imag * scales[index]))
            else:
                state[index] = jnp.where(
                    is_real,
                    jnp.broadcast_to(new_real, (8, dates)),
                    jnp.where(is_imag, jnp.broadcast_to(new_imag, (8, dates)), 0.0),
                )
    return result


def descending(count, me):
    return [top - (top <= me).astype(jnp.int32) for top in range(count - 1, 0, -1)]


def at_distance(count, me, distance):
    pairs = count // PAIR
    row, side = me // PAIR, lax.rem(me, PAIR)
    found = []
    for across in range(PAIR):
        steps = distance - across
        if steps < 0:
            continue
        for along in sorted({steps, -steps}, reverse=True):
            if abs(along) < pairs:
                exists = jnp.logical_and(row + along >= 0, row + along < pairs)
                found.append((exists, (row + along) * PAIR + (1 - side if across else side)))
    return found


def kernel(
    count, looks_count, windows,
    slc_hbm, usable_hbm, coherence_ref, linked_ref,
    slc_ref, usable_ref, packed, arrived, vectors, turned, landed,
    in_sem, send_sem, recv_sem, back_send, back_recv, round_sem,
):
    me = lax.axis_index("date")
    core = jnp.minimum(lax.axis_index("sub"), len(SENT) - 1)
    own, local_windows = usable_ref.shape[1:]
    dates = count * own
    span = LANES // QUAD
    full = looks_count // span
    rest = looks_count - full * span
    parts = windows // QUAD
    extra = packed.shape[1] - 2 * full * parts
    later = 2 * (full - 1)
    tile_owners = LANES // windows

    barrier = pltpu.get_barrier_semaphore()
    farthest = count // PAIR - 1 + PAIR - 1
    beside = at_distance(count, me, 1)
    greetings = sum(exists.astype(jnp.int32) for exists, _ in beside)

    def greet(semaphore):
        for exists, other in beside:
            @pl.when(exists)
            def _():
                pl.semaphore_signal(
                    semaphore, inc=1, device_id={"date": other}, device_id_type=pl.DeviceIdType.MESH
                )

    greet(barrier)

    chunks = [(0, span)] + ([(full * span, rest)] if rest else [])
    chunks += [(index * span, span) for index in range(1, full)]

    def loads(index):
        start, size = chunks[index]
        looks = pl.ds(start, size)
        return (
            pltpu.make_async_copy(usable_hbm.at[looks], usable_ref.at[looks], in_sem.at[index, 0]),
            pltpu.make_async_copy(slc_hbm.at[:, looks], slc_ref.at[:, looks], in_sem.at[index, 1]),
        )

    for index in range(len(chunks)):
        for copy in loads(index):
            copy.start()

    def masked(side, look, tile):
        lanes = slice(tile * LANES, (tile + 1) * LANES)
        return slc_ref[side, look, :, lanes] * usable_ref[look, :, lanes].astype(jnp.float32).astype(jnp.bfloat16)

    def first_block(part, side):
        return 2 * part + side

    def later_block(part, side, index):
        return 2 * parts + extra + part * later + side * (full - 1) + index - 1

    tiles = local_windows // LANES

    def prepare(index):
        start, size = chunks[index]
        for copy in loads(index):
            copy.wait()
        for tile in range(tiles):
            if size == span:
                for side in range(2):
                    blocks = swap_strips([masked(side, start + look, tile) for look in range(span)], False)
                    for place, block in enumerate(blocks):
                        owner, part = divmod(place, parts)
                        row = later_block(part, side, start // span) if start else first_block(part, side)
                        packed[tile * tile_owners + owner, row] = block
            else:
                half = tile_owners // 2
                zero = jnp.zeros((own, LANES), jnp.bfloat16)
                for piece in range(extra):
                    blocks = swap_strips(
                        [
                            masked(side, start + piece * half + look, tile) if piece * half + look < size else zero
                            for side in range(2)
                            for look in range(half)
                        ],
                        True,
                    )
                    for owner, block in enumerate(blocks):
                        packed[tile * tile_owners + owner, 2 * parts + piece] = block

    others = descending(count, me)

    def blocks_of(message):
        if message == 0:
            return pl.ds(0, 2 * parts)
        if message == 1:
            return pl.ds(2 * parts, extra + later)
        return pl.ds(2 * parts + extra + (message - 1) * later, later)

    def block_copy(message, other, source):
        return pltpu.make_async_remote_copy(
            src_ref=packed.at[other, blocks_of(message)],
            dst_ref=arrived.at[source, blocks_of(message)],
            send_sem=send_sem.at[message, other],
            recv_sem=recv_sem.at[message, source],
            device_id={"date": other},
            device_id_type=pl.DeviceIdType.MESH,
        )

    def send_at(distance, messages):
        for exists, other in at_distance(count, me, distance):
            @pl.when(exists)
            def _():
                for message in messages:
                    block_copy(message, other, me).start()

    def send_all(message):
        for other in others:
            block_copy(message, other, me).start()

    with jax.named_scope("prepare_first"):
        prepare(0)
    with jax.named_scope("meet_first"):
        pl.semaphore_wait(barrier, greetings)
    if farthest > 1:
        greet(round_sem.at[0])
    send_at(1, [0])
    with jax.named_scope("prepare_rest"):
        for index in range(1, len(chunks)):
            prepare(index)
    send_at(1, [1])
    for distance in range(2, farthest + 1):
        with jax.named_scope("meet_next"):
            pl.semaphore_wait(round_sem.at[distance - 2], greetings)
        if distance < farthest:
            greet(round_sem.at[distance - 1])
        send_at(distance, [0, 1])
    def send_paced(arrived_parts):
        for index, counts in enumerate(SENT):
            first = counts[min(arrived_parts - 1, len(counts) - 1)] if arrived_parts else 2
            messages = range(first, min(counts[min(arrived_parts, len(counts) - 1)], parts + 1))
            if messages:
                @pl.when(core == index)
                def _():
                    for message in messages:
                        send_all(message)

    send_paced(0)
    arrived[me] = packed[me]

    lane = lax.broadcasted_iota(jnp.int32, (2 * dates, LANES), 1)

    def compute_part(part):
        with jax.named_scope(f"wait_{part}"):
            for message in range(0 if part == 0 else part + 1, part + 2):
                for other in others:
                    block_copy(message, other, other).wait_recv()
        send_paced(part + 1)

        def gathered(block):
            return arrived[:, block].reshape(dates, LANES)

        columns = []
        for piece in range(extra):
            both = gathered(2 * parts + piece)
            columns.append((jnp.concatenate([both, pltpu.roll(both, LANES // 2, 1)], axis=0), True))
        for index in range(full):
            sides = [
                gathered(later_block(part, side, index) if index else first_block(part, side)) for side in range(2)
            ]
            columns.append((jnp.concatenate(sides, axis=0), False))
        right = jnp.concatenate([block for block, _ in columns], axis=1)
        matrices = []
        for inner in range(QUAD):
            window = part * QUAD + inner
            mine = jnp.logical_and(lane < LANES // 2, (lane & (windows - 1)) == window)
            own_lane = (lane & (QUAD - 1)) == inner
            left = jnp.concatenate(
                [jnp.where(mine if shared else own_lane, block, jnp.zeros_like(block)) for block, shared in columns],
                axis=1,
            )
            real, imag = window_coherence(dot_nt(left, right), looks_count)
            coherence_ref[0, 0, 0, window] = real
            coherence_ref[1, 0, 0, window] = imag
            matrices.append(jnp.concatenate([real, imag], axis=1))
        for inner, (real, imag) in enumerate(link_windows(matrices)):
            vectors[0, pl.ds(part * QUAD + inner, 1)] = real
            vectors[1, pl.ds(part * QUAD + inner, 1)] = imag

    for part in range(parts):
        with jax.named_scope(f"part_{part}"):
            compute_part(part)

    fold, rows, width = own // turned.shape[1], turned.shape[1], 2 * windows
    spread = jnp.concatenate([vectors[0], vectors[1]], axis=0)
    spread = jnp.pad(spread, ((0, LANES - width), (0, 0))).T.reshape(count, fold, rows, LANES)
    folded = spread[:, 0]
    for place in range(1, fold):
        folded = folded + pltpu.roll(
            spread[:, place].reshape(count * rows, LANES), place * width, 1
        ).reshape(count, rows, LANES)
    turned[...] = folded

    def back_copy(other, source):
        return pltpu.make_async_remote_copy(
            src_ref=turned.at[other],
            dst_ref=landed.at[source],
            send_sem=back_send.at[other],
            recv_sem=back_recv.at[source],
            device_id={"date": other},
            device_id_type=pl.DeviceIdType.MESH,
        )

    for other in reversed(others):
        back_copy(other, me).start()
    landed[me] = turned[me]
    with jax.named_scope("wait_back"):
        for other in others:
            back_copy(other, other).wait_recv()
    for side in range(2):
        for place in range(fold):
            first = place * width + side * windows
            linked_ref[side, place * rows : (place + 1) * rows] = jnp.concatenate(
                [landed[source][:, first : first + windows] for source in range(count)], axis=1
            )

    for message in range(parts + 1):
        for other in others:
            block_copy(message, other, me).wait_send()
    for other in others:
        back_copy(other, me).wait_send()


def deliver(coherence_in, linked_in, coherence_out, linked_out, sem):
    copies = [pltpu.make_async_copy(linked_in, linked_out, sem.at[0])]
    windows = coherence_in.shape[3]
    pieces = PIECES if windows % PIECES == 0 else 1
    size = windows // pieces
    for side in range(coherence_in.shape[0]):
        for piece in range(pieces):
            span = pl.ds(piece * size, size)
            copies.append(
                pltpu.make_async_copy(
                    coherence_in.at[side, :, :, span],
                    coherence_out.at[side, :, :, span],
                    sem.at[1 + side * PIECES + piece],
                )
            )
    for copy in copies:
        copy.start()
    for copy in copies:
        copy.wait()


def local(slc, usable):
    looks_count, own_dates, windows = usable.shape
    count = lax.axis_size("date")
    per_device = windows // count
    dates = own_dates * count
    parts = per_device // QUAD
    span = LANES // QUAD
    full = looks_count // span
    extra = pl.cdiv(looks_count - full * span, LANES // per_device // 2)
    fold = max(1, own_dates // 8)
    fold = fold if own_dates % fold == 0 and 2 * per_device * fold <= LANES else 1
    blocks = extra + 2 * full * parts
    results = pl.pallas_call(
        functools.partial(kernel, count, looks_count, per_device),
        out_shape=(
            jax.ShapeDtypeStruct((2, 1, 1, per_device, dates, dates), jnp.bfloat16),
            jax.ShapeDtypeStruct((2, own_dates, windows), jnp.float32),
        ),
        in_specs=[pl.BlockSpec(memory_space=pltpu.HBM)] * 2,
        out_specs=(
            pl.BlockSpec(memory_space=pltpu.VMEM),
            pl.BlockSpec(memory_space=pltpu.VMEM),
        ),
        scratch_shapes=[
            pltpu.VMEM((2, looks_count, own_dates, windows), jnp.bfloat16),
            pltpu.VMEM((looks_count, own_dates, windows), jnp.int32),
            pltpu.VMEM((count, blocks, own_dates, LANES), jnp.bfloat16),
            pltpu.VMEM((count, blocks, own_dates, LANES), jnp.bfloat16),
            pltpu.VMEM((2, per_device, dates), jnp.float32),
            pltpu.VMEM((count, own_dates // fold, LANES), jnp.float32),
            pltpu.VMEM((count, own_dates // fold, LANES), jnp.float32),
            pltpu.SemaphoreType.DMA((full + 1, 2)),
            pltpu.SemaphoreType.DMA((parts + 1, count)),
            pltpu.SemaphoreType.DMA((parts + 1, count)),
            pltpu.SemaphoreType.DMA((count,)),
            pltpu.SemaphoreType.DMA((count,)),
            pltpu.SemaphoreType.REGULAR((count // PAIR + PAIR - 2,)),
        ],
        compiler_params=pltpu.CompilerParams(collective_id=0, has_side_effects=True, vmem_limit_bytes=24 << 20),
    )(pltpu.with_memory_space_constraint(slc, pltpu.HBM), pltpu.with_memory_space_constraint(usable, pltpu.HBM))
    return pl.pallas_call(
        deliver,
        out_shape=tuple(jax.ShapeDtypeStruct(array.shape, array.dtype) for array in results),
        in_specs=[pl.BlockSpec(memory_space=pl.ANY)] * 2,
        out_specs=(pl.BlockSpec(memory_space=pl.ANY),) * 2,
        scratch_shapes=[pltpu.SemaphoreType.DMA((results[0].shape[0] * PIECES + 1,))],
        compiler_params=pltpu.CompilerParams(vmem_limit_bytes=1 << 20),
    )(*results)


def solution(mesh):
    return jax.shard_map(
        local,
        mesh=mesh,
        in_specs=(
            P(None, None, "date", ("slab", "tile", "sub")),
            P(None, "date", ("slab", "tile", "sub")),
        ),
        out_specs=(
            P(None, ("slab", "tile", "sub"), "date", None, None, None),
            P(None, "date", ("slab", "tile", "sub")),
        ),
        check_vma=False,
    )
```

```python
import functools

import jax
import jax.numpy as jnp
from jax import lax
from jax.experimental import pallas as pl
from jax.experimental.pallas import tpu as pltpu
from jax.sharding import PartitionSpec as P

ITERS = 4
LANES = 128
QUAD = 4
PAIR = 2

SENT = ((4, 5), (2, 4, 5))
PIECES = 2
NT = (((1,), (1,)), ((), ()))


def dot_nt(left, right):
    return lax.dot_general(left, right, NT, preferred_element_type=jnp.float32)


def lane_bit(rows, strip):
    return (lax.broadcasted_iota(jnp.int32, (rows, LANES), 1) & strip) != 0


def swap_strips(blocks, exact):
    blocks = list(blocks)
    bit, strip = len(blocks) // 2, LANES // 2
    while bit:
        high = lane_bit(blocks[0].shape[0], strip)
        for low_index in range(len(blocks)):
            if low_index & bit:
                continue
            first, second = blocks[low_index], blocks[low_index | bit]
            if exact and strip != LANES // 2:
                blocks[low_index] = jnp.where(high, pltpu.roll(second, strip, 1), first)
                blocks[low_index | bit] = jnp.where(high, second, pltpu.roll(first, LANES - strip, 1))
            else:
                moved = pltpu.roll(jnp.where(high, first, second), strip, 1)
                blocks[low_index] = jnp.where(high, moved, first)
                blocks[low_index | bit] = jnp.where(high, second, moved)
        bit, strip = bit // 2, strip // 2
    return blocks


def cross_sums(left, right):
    sums = dot_nt(left, right)
    dates = sums.shape[0] // 2
    return sums[:dates, :dates] + sums[dates:, dates:], sums[dates:, :dates] - sums[:dates, dates:]


def window_coherence(real_sum, imag_sum, looks_count):
    dates = real_sum.shape[0]
    rows = lax.broadcasted_iota(jnp.int32, (dates, dates), 0)
    columns = lax.broadcasted_iota(jnp.int32, (dates, dates), 1)
    diagonal = jnp.where(rows == columns, real_sum, 0.0)
    row_root = lax.rsqrt(jnp.sum(diagonal, axis=0, keepdims=True) * (1.0 / looks_count) + 1e-05)
    column_root = lax.rsqrt(jnp.sum(diagonal, axis=1, keepdims=True) * (1.0 / looks_count) + 1e-05)
    factor = column_root * row_root * (1.0 / looks_count)
    return (real_sum * factor).astype(jnp.bfloat16), (imag_sum * factor).astype(jnp.bfloat16)


def link_windows(matrices):
    dates = matrices[0].shape[0]
    row = lax.broadcasted_iota(jnp.int32, (8, dates), 0)
    is_real = row < 3
    is_imag = jnp.logical_and(row >= 3, row < 6)
    is_first = jnp.logical_or(row == 0, row == 3)
    is_second = jnp.logical_or(row == 1, row == 4)
    state, scales = [None] * len(matrices), [None] * len(matrices)
    result = []
    for step in range(ITERS):
        products = [None] * len(matrices)
        for index, (vec, matrix) in enumerate(zip(state, matrices) if step else ()):
            high = vec.astype(jnp.bfloat16).astype(jnp.float32)
            left = vec - high
            middle = left.astype(jnp.bfloat16).astype(jnp.float32)
            pieces = jnp.where(is_first, high, jnp.where(is_second, middle, left - middle))
            products[index] = jnp.dot(pieces.astype(jnp.bfloat16), matrix, preferred_element_type=jnp.float32)
        for index, product in enumerate(products):
            if step:
                first, second = product[:, :dates], product[:, dates:]
                zero = jnp.zeros_like(first)
                new_real = jnp.sum(
                    jnp.where(is_real, first, jnp.where(is_imag, second, zero)), axis=0, keepdims=True
                )
                new_imag = jnp.sum(
                    jnp.where(is_real, -second, jnp.where(is_imag, first, zero)), axis=0, keepdims=True
                )
                new_real = new_real * scales[index]
                new_imag = new_imag * scales[index]
            else:
                sums = jnp.sum(matrices[index].astype(jnp.float32), axis=0, keepdims=True)
                new_real, new_imag = sums[:, :dates], -sums[:, dates:]
            power = jnp.sum(new_real * new_real + new_imag * new_imag, axis=1, keepdims=True)
            scales[index] = lax.rsqrt(power * (1.0 / dates) + 1e-05)
            if step == ITERS - 1:
                result.append((new_real * scales[index], new_imag * scales[index]))
            else:
                state[index] = jnp.where(
                    is_real,
                    jnp.broadcast_to(new_real, (8, dates)),
                    jnp.where(is_imag, jnp.broadcast_to(new_imag, (8, dates)), 0.0),
                )
    return result


def descending(count, me):
    return [top - (top <= me).astype(jnp.int32) for top in range(count - 1, 0, -1)]


def at_distance(count, me, distance):
    pairs = count // PAIR
    row, side = me // PAIR, lax.rem(me, PAIR)
    found = []
    for across in range(PAIR):
        steps = distance - across
        if steps < 0:
            continue
        for along in sorted({steps, -steps}, reverse=True):
            if abs(along) < pairs:
                exists = jnp.logical_and(row + along >= 0, row + along < pairs)
                found.append((exists, (row + along) * PAIR + (1 - side if across else side)))
    return found


def kernel(
    count, looks_count, windows,
    slc_hbm, usable_hbm, coherence_ref, linked_ref,
    slc_ref, usable_ref, packed, arrived, vectors, turned, landed,
    in_sem, send_sem, recv_sem, back_send, back_recv, round_sem, partial,
):
    me = lax.axis_index("date")
    core = jnp.minimum(lax.axis_index("sub"), len(SENT) - 1)
    own, local_windows = usable_ref.shape[1:]
    dates = count * own
    span = LANES // QUAD
    full = looks_count // span
    rest = looks_count - full * span
    parts = windows // QUAD
    extra = packed.shape[1] - 2 * full * parts
    later = 2 * (full - 1)
    tile_owners = LANES // windows

    barrier = pltpu.get_barrier_semaphore()
    farthest = count // PAIR - 1 + PAIR - 1
    beside = at_distance(count, me, 1)
    greetings = sum(exists.astype(jnp.int32) for exists, _ in beside)

    def greet(semaphore):
        for exists, other in beside:
            @pl.when(exists)
            def _():
                pl.semaphore_signal(
                    semaphore, inc=1, device_id={"date": other}, device_id_type=pl.DeviceIdType.MESH
                )

    greet(barrier)

    chunks = [(0, span)] + ([(full * span, rest)] if rest else [])
    chunks += [(index * span, span) for index in range(1, full)]

    def loads(index):
        start, size = chunks[index]
        looks = pl.ds(start, size)
        return (
            pltpu.make_async_copy(usable_hbm.at[looks], usable_ref.at[looks], in_sem.at[index, 0]),
            pltpu.make_async_copy(slc_hbm.at[:, looks], slc_ref.at[:, looks], in_sem.at[index, 1]),
        )

    for index in range(len(chunks)):
        for copy in loads(index):
            copy.start()

    def masked(side, look, tile):
        lanes = slice(tile * LANES, (tile + 1) * LANES)
        return slc_ref[side, look, :, lanes] * usable_ref[look, :, lanes].astype(jnp.float32).astype(jnp.bfloat16)

    def first_block(part, side):
        return 2 * part + side

    def later_block(part, side, index):
        return 2 * parts + extra + part * later + side * (full - 1) + index - 1

    tiles = local_windows // LANES

    def prepare(index):
        start, size = chunks[index]
        for copy in loads(index):
            copy.wait()
        for tile in range(tiles):
            if size == span:
                for side in range(2):
                    blocks = swap_strips([masked(side, start + look, tile) for look in range(span)], False)
                    for place, block in enumerate(blocks):
                        owner, part = divmod(place, parts)
                        row = later_block(part, side, start // span) if start else first_block(part, side)
                        packed[tile * tile_owners + owner, row] = block
            else:
                half = tile_owners // 2
                zero = jnp.zeros((own, LANES), jnp.bfloat16)
                for piece in range(extra):
                    blocks = swap_strips(
                        [
                            masked(side, start + piece * half + look, tile) if piece * half + look < size else zero
                            for side in range(2)
                            for look in range(half)
                        ],
                        True,
                    )
                    for owner, block in enumerate(blocks):
                        packed[tile * tile_owners + owner, 2 * parts + piece] = block

    others = descending(count, me)

    def blocks_of(message):
        if message == 0:
            return pl.ds(0, 2 * parts)
        if message == 1:
            return pl.ds(2 * parts, extra + later)
        return pl.ds(2 * parts + extra + (message - 1) * later, later)

    def block_copy(message, other, source):
        return pltpu.make_async_remote_copy(
            src_ref=packed.at[other, blocks_of(message)],
            dst_ref=arrived.at[source, blocks_of(message)],
            send_sem=send_sem.at[message, other],
            recv_sem=recv_sem.at[message, source],
            device_id={"date": other},
            device_id_type=pl.DeviceIdType.MESH,
        )

    def send_at(distance, messages):
        for exists, other in at_distance(count, me, distance):
            @pl.when(exists)
            def _():
                for message in messages:
                    block_copy(message, other, me).start()

    def send_all(message):
        for other in others if message == parts else reversed(others):
            block_copy(message, other, me).start()

    with jax.named_scope("prepare_first"):
        prepare(0)
    with jax.named_scope("meet_first"):
        pl.semaphore_wait(barrier, greetings)
    if farthest > 1:
        greet(round_sem.at[0])
    send_at(1, [0])
    with jax.named_scope("prepare_rest"):
        for index in range(1, len(chunks)):
            prepare(index)
    send_at(1, [1])
    for distance in range(2, farthest + 1):
        with jax.named_scope("meet_next"):
            pl.semaphore_wait(round_sem.at[distance - 2], greetings)
        if distance < farthest:
            greet(round_sem.at[distance - 1])
        send_at(distance, [0, 1])
    def send_paced(arrived_parts):
        for index, counts in enumerate(SENT):
            first = counts[min(arrived_parts - 1, len(counts) - 1)] if arrived_parts else 2
            messages = range(first, min(counts[min(arrived_parts, len(counts) - 1)], parts + 1))
            if messages:
                @pl.when(core == index)
                def _():
                    for message in messages:
                        send_all(message)

    send_paced(0)
    arrived[me] = packed[me]

    lane = lax.broadcasted_iota(jnp.int32, (2 * dates, LANES), 1)

    def gathered(block):
        return arrived[:, block].reshape(dates, LANES)

    def shared_columns():
        columns = []
        for piece in range(extra):
            both = gathered(2 * parts + piece)
            columns.append((jnp.concatenate([both, pltpu.roll(both, LANES // 2, 1)], axis=0), True))
        return columns

    def span_columns(part, spans):
        columns = []
        for index in spans:
            sides = [
                gathered(later_block(part, side, index) if index else first_block(part, side)) for side in range(2)
            ]
            columns.append((jnp.concatenate(sides, axis=0), False))
        return columns

    def windows_sums(part, columns):
        right = jnp.concatenate([block for block, _ in columns], axis=1)
        for inner in range(QUAD):
            mine = jnp.logical_and(lane < LANES // 2, (lane & (windows - 1)) == part * QUAD + inner)
            own_lane = (lane & (QUAD - 1)) == inner
            left = jnp.concatenate(
                [jnp.where(mine if shared else own_lane, block, jnp.zeros_like(block)) for block, shared in columns],
                axis=1,
            )
            yield cross_sums(left, right)

    def sum_ahead(part):
        for inner, sums in enumerate(windows_sums(part, shared_columns() + span_columns(part, [0]))):
            partial[inner, 0], partial[inner, 1] = sums

    def compute_part(part, ahead):
        with jax.named_scope(f"wait_{part}"):
            for message in range(0 if part == 0 else part + 1, part + 2):
                for other in others:
                    block_copy(message, other, other).wait_recv()
        send_paced(part + 1)
        columns = span_columns(part, range(1, full)) if ahead else shared_columns() + span_columns(part, range(full))
        matrices = []
        for inner, (real_sum, imag_sum) in enumerate(windows_sums(part, columns)):
            window = part * QUAD + inner
            if ahead:
                real_sum, imag_sum = real_sum + partial[inner, 0], imag_sum + partial[inner, 1]
            real, imag = window_coherence(real_sum, imag_sum, looks_count)
            coherence_ref[0, 0, 0, window] = real
            coherence_ref[1, 0, 0, window] = imag
            matrices.append(jnp.concatenate([real, imag], axis=1))
        for inner, (real, imag) in enumerate(link_windows(matrices)):
            vectors[0, pl.ds(part * QUAD + inner, 1)] = real
            vectors[1, pl.ds(part * QUAD + inner, 1)] = imag

    for part in range(parts):
        with jax.named_scope(f"part_{part}"):
            ahead = 0 < part == parts - 1 and full > 1
            if ahead:
                sum_ahead(part)
            compute_part(part, ahead)

    fold, rows, width = own // turned.shape[1], turned.shape[1], 2 * windows
    spread = jnp.concatenate([vectors[0], vectors[1]], axis=0)
    spread = jnp.pad(spread, ((0, LANES - width), (0, 0))).T.reshape(count, fold, rows, LANES)
    folded = spread[:, 0]
    for place in range(1, fold):
        folded = folded + pltpu.roll(
            spread[:, place].reshape(count * rows, LANES), place * width, 1
        ).reshape(count, rows, LANES)
    turned[...] = folded

    def back_copy(other, source):
        return pltpu.make_async_remote_copy(
            src_ref=turned.at[other],
            dst_ref=landed.at[source],
            send_sem=back_send.at[other],
            recv_sem=back_recv.at[source],
            device_id={"date": other},
            device_id_type=pl.DeviceIdType.MESH,
        )

    for other in reversed(others):
        back_copy(other, me).start()
    landed[me] = turned[me]
    with jax.named_scope("wait_back"):
        for other in others:
            back_copy(other, other).wait_recv()
    for side in range(2):
        for place in range(fold):
            first = place * width + side * windows
            linked_ref[side, place * rows : (place + 1) * rows] = jnp.concatenate(
                [landed[source][:, first : first + windows] for source in range(count)], axis=1
            )

    for message in range(parts + 1):
        for other in others:
            block_copy(message, other, me).wait_send()
    for other in others:
        back_copy(other, me).wait_send()


def deliver(coherence_in, linked_in, coherence_out, linked_out, sem):
    copies = [pltpu.make_async_copy(linked_in, linked_out, sem.at[0])]
    windows = coherence_in.shape[3]
    pieces = PIECES if windows % PIECES == 0 else 1
    size = windows // pieces
    for side in range(coherence_in.shape[0]):
        for piece in range(pieces):
            span = pl.ds(piece * size, size)
            copies.append(
                pltpu.make_async_copy(
                    coherence_in.at[side, :, :, span],
                    coherence_out.at[side, :, :, span],
                    sem.at[1 + side * PIECES + piece],
                )
            )
    for copy in copies:
        copy.start()
    for copy in copies:
        copy.wait()


def local(slc, usable):
    looks_count, own_dates, windows = usable.shape
    count = lax.axis_size("date")
    per_device = windows // count
    dates = own_dates * count
    parts = per_device // QUAD
    span = LANES // QUAD
    full = looks_count // span
    extra = pl.cdiv(looks_count - full * span, LANES // per_device // 2)
    fold = max(1, own_dates // 8)
    fold = fold if own_dates % fold == 0 and 2 * per_device * fold <= LANES else 1
    blocks = extra + 2 * full * parts
    results = pl.pallas_call(
        functools.partial(kernel, count, looks_count, per_device),
        out_shape=(
            jax.ShapeDtypeStruct((2, 1, 1, per_device, dates, dates), jnp.bfloat16),
            jax.ShapeDtypeStruct((2, own_dates, windows), jnp.float32),
        ),
        in_specs=[pl.BlockSpec(memory_space=pltpu.HBM)] * 2,
        out_specs=(
            pl.BlockSpec(memory_space=pltpu.VMEM),
            pl.BlockSpec(memory_space=pltpu.VMEM),
        ),
        scratch_shapes=[
            pltpu.VMEM((2, looks_count, own_dates, windows), jnp.bfloat16),
            pltpu.VMEM((looks_count, own_dates, windows), jnp.int32),
            pltpu.VMEM((count, blocks, own_dates, LANES), jnp.bfloat16),
            pltpu.VMEM((count, blocks, own_dates, LANES), jnp.bfloat16),
            pltpu.VMEM((2, per_device, dates), jnp.float32),
            pltpu.VMEM((count, own_dates // fold, LANES), jnp.float32),
            pltpu.VMEM((count, own_dates // fold, LANES), jnp.float32),
            pltpu.SemaphoreType.DMA((full + 1, 2)),
            pltpu.SemaphoreType.DMA((parts + 1, count)),
            pltpu.SemaphoreType.DMA((parts + 1, count)),
            pltpu.SemaphoreType.DMA((count,)),
            pltpu.SemaphoreType.DMA((count,)),
            pltpu.SemaphoreType.REGULAR((count // PAIR + PAIR - 2,)),
            pltpu.VMEM((QUAD, 2, dates, dates), jnp.float32),
        ],
        compiler_params=pltpu.CompilerParams(collective_id=0, has_side_effects=True, vmem_limit_bytes=24 << 20),
    )(pltpu.with_memory_space_constraint(slc, pltpu.HBM), pltpu.with_memory_space_constraint(usable, pltpu.HBM))
    return pl.pallas_call(
        deliver,
        out_shape=tuple(jax.ShapeDtypeStruct(array.shape, array.dtype) for array in results),
        in_specs=[pl.BlockSpec(memory_space=pl.ANY)] * 2,
        out_specs=(pl.BlockSpec(memory_space=pl.ANY),) * 2,
        scratch_shapes=[pltpu.SemaphoreType.DMA((results[0].shape[0] * PIECES + 1,))],
        compiler_params=pltpu.CompilerParams(vmem_limit_bytes=1 << 20),
    )(*results)


def solution(mesh):
    return jax.shard_map(
        local,
        mesh=mesh,
        in_specs=(
            P(None, None, "date", ("slab", "tile", "sub")),
            P(None, "date", ("slab", "tile", "sub")),
        ),
        out_specs=(
            P(None, ("slab", "tile", "sub"), "date", None, None, None),
            P(None, "date", ("slab", "tile", "sub")),
        ),
        check_vma=False,
    )
```

```python
import functools

import jax
import jax.numpy as jnp
from jax import lax
from jax.experimental import pallas as pl
from jax.experimental.pallas import tpu as pltpu
from jax.sharding import PartitionSpec as P

ITERS = 4
LANES = 128
QUAD = 4
PAIR = 2

SENT = ((4, 5), (2, 4, 5))
PIECES = 2
NT = (((1,), (1,)), ((), ()))


def dot_nt(left, right):
    return lax.dot_general(left, right, NT, preferred_element_type=jnp.float32)


def lane_bit(rows, strip):
    return (lax.broadcasted_iota(jnp.int32, (rows, LANES), 1) & strip) != 0


def swap_strips(blocks, exact):
    blocks = list(blocks)
    bit, strip = len(blocks) // 2, LANES // 2
    while bit:
        high = lane_bit(blocks[0].shape[0], strip)
        for low_index in range(len(blocks)):
            if low_index & bit:
                continue
            first, second = blocks[low_index], blocks[low_index | bit]
            if exact and strip != LANES // 2:
                blocks[low_index] = jnp.where(high, pltpu.roll(second, strip, 1), first)
                blocks[low_index | bit] = jnp.where(high, second, pltpu.roll(first, LANES - strip, 1))
            else:
                moved = pltpu.roll(jnp.where(high, first, second), strip, 1)
                blocks[low_index] = jnp.where(high, moved, first)
                blocks[low_index | bit] = jnp.where(high, second, moved)
        bit, strip = bit // 2, strip // 2
    return blocks


def cross_sums(left, right):
    sums = dot_nt(left, right)
    dates = sums.shape[0] // 2
    return sums[:dates, :dates] + sums[dates:, dates:], sums[dates:, :dates] - sums[:dates, dates:]


def window_coherence(real_sum, imag_sum, looks_count):
    dates = real_sum.shape[0]
    rows = lax.broadcasted_iota(jnp.int32, (dates, dates), 0)
    columns = lax.broadcasted_iota(jnp.int32, (dates, dates), 1)
    diagonal = jnp.where(rows == columns, real_sum, 0.0)
    row_root = lax.rsqrt(jnp.sum(diagonal, axis=0, keepdims=True) * (1.0 / looks_count) + 1e-05)
    column_root = lax.rsqrt(jnp.sum(diagonal, axis=1, keepdims=True) * (1.0 / looks_count) + 1e-05)
    factor = column_root * row_root * (1.0 / looks_count)
    return (real_sum * factor).astype(jnp.bfloat16), (imag_sum * factor).astype(jnp.bfloat16)


def link_windows(matrices):
    dates = matrices[0].shape[0]
    row = lax.broadcasted_iota(jnp.int32, (8, dates), 0)
    is_real = row < 3
    is_imag = jnp.logical_and(row >= 3, row < 6)
    is_first = jnp.logical_or(row == 0, row == 3)
    is_second = jnp.logical_or(row == 1, row == 4)
    state, scales = [None] * len(matrices), [None] * len(matrices)
    result = []
    for step in range(ITERS):
        products = [None] * len(matrices)
        for index, (vec, matrix) in enumerate(zip(state, matrices) if step else ()):
            high = vec.astype(jnp.bfloat16).astype(jnp.float32)
            left = vec - high
            middle = left.astype(jnp.bfloat16).astype(jnp.float32)
            pieces = jnp.where(is_first, high, jnp.where(is_second, middle, left - middle))
            products[index] = jnp.dot(pieces.astype(jnp.bfloat16), matrix, preferred_element_type=jnp.float32)
        for index, product in enumerate(products):
            if step:
                first, second = product[:, :dates], product[:, dates:]
                zero = jnp.zeros_like(first)
                new_real = jnp.sum(
                    jnp.where(is_real, first, jnp.where(is_imag, second, zero)), axis=0, keepdims=True
                )
                new_imag = jnp.sum(
                    jnp.where(is_real, -second, jnp.where(is_imag, first, zero)), axis=0, keepdims=True
                )
                new_real = new_real * scales[index]
                new_imag = new_imag * scales[index]
            else:
                sums = jnp.sum(matrices[index].astype(jnp.float32), axis=0, keepdims=True)
                new_real, new_imag = sums[:, :dates], -sums[:, dates:]
            power = jnp.sum(new_real * new_real + new_imag * new_imag, axis=1, keepdims=True)
            scales[index] = lax.rsqrt(power * (1.0 / dates) + 1e-05)
            if step == ITERS - 1:
                result.append((new_real * scales[index], new_imag * scales[index]))
            else:
                state[index] = jnp.where(
                    is_real,
                    jnp.broadcast_to(new_real, (8, dates)),
                    jnp.where(is_imag, jnp.broadcast_to(new_imag, (8, dates)), 0.0),
                )
    return result


def descending(count, me):
    return [top - (top <= me).astype(jnp.int32) for top in range(count - 1, 0, -1)]


def at_distance(count, me, distance):
    pairs = count // PAIR
    row, side = me // PAIR, lax.rem(me, PAIR)
    found = []
    for across in range(PAIR):
        steps = distance - across
        if steps < 0:
            continue
        for along in sorted({steps, -steps}, reverse=True):
            if abs(along) < pairs:
                exists = jnp.logical_and(row + along >= 0, row + along < pairs)
                found.append((exists, (row + along) * PAIR + (1 - side if across else side)))
    return found


def kernel(
    count, looks_count, windows,
    slc_hbm, usable_hbm, coherence_ref, linked_ref,
    slc_ref, usable_ref, packed, arrived, vectors, turned, landed,
    in_sem, send_sem, recv_sem, back_send, back_recv, round_sem, partial,
):
    me = lax.axis_index("date")
    core = jnp.minimum(lax.axis_index("sub"), len(SENT) - 1)
    own, local_windows = usable_ref.shape[1:]
    dates = count * own
    span = LANES // QUAD
    full = looks_count // span
    rest = looks_count - full * span
    parts = windows // QUAD
    extra = packed.shape[1] - 2 * full * parts
    later = 2 * (full - 1)
    tile_owners = LANES // windows

    barrier = pltpu.get_barrier_semaphore()
    farthest = count // PAIR - 1 + PAIR - 1
    beside = at_distance(count, me, 1)
    greetings = sum(exists.astype(jnp.int32) for exists, _ in beside)

    def greet(semaphore):
        for exists, other in beside:
            @pl.when(exists)
            def _():
                pl.semaphore_signal(
                    semaphore, inc=1, device_id={"date": other}, device_id_type=pl.DeviceIdType.MESH
                )

    greet(barrier)

    chunks = [(0, span)] + ([(full * span, rest)] if rest else [])
    chunks += [(index * span, span) for index in range(1, full)]

    def loads(index):
        start, size = chunks[index]
        looks = pl.ds(start, size)
        return (
            pltpu.make_async_copy(usable_hbm.at[looks], usable_ref.at[looks], in_sem.at[index, 0]),
            pltpu.make_async_copy(slc_hbm.at[:, looks], slc_ref.at[:, looks], in_sem.at[index, 1]),
        )

    for index in range(len(chunks)):
        for copy in loads(index):
            copy.start()

    def masked(side, look, tile):
        lanes = slice(tile * LANES, (tile + 1) * LANES)
        return slc_ref[side, look, :, lanes] * usable_ref[look, :, lanes].astype(jnp.float32).astype(jnp.bfloat16)

    def first_block(part, side):
        return 2 * part + side

    def later_block(part, side, index):
        return 2 * parts + extra + part * later + side * (full - 1) + index - 1

    tiles = local_windows // LANES

    def prepare(index):
        start, size = chunks[index]
        for copy in loads(index):
            copy.wait()
        for tile in range(tiles):
            if size == span:
                for side in range(2):
                    blocks = swap_strips([masked(side, start + look, tile) for look in range(span)], False)
                    for place, block in enumerate(blocks):
                        owner, part = divmod(place, parts)
                        row = later_block(part, side, start // span) if start else first_block(part, side)
                        packed[tile * tile_owners + owner, row] = block
            else:
                half = tile_owners // 2
                zero = jnp.zeros((own, LANES), jnp.bfloat16)
                for piece in range(extra):
                    blocks = swap_strips(
                        [
                            masked(side, start + piece * half + look, tile) if piece * half + look < size else zero
                            for side in range(2)
                            for look in range(half)
                        ],
                        True,
                    )
                    for owner, block in enumerate(blocks):
                        packed[tile * tile_owners + owner, 2 * parts + piece] = block

    others = descending(count, me)

    def blocks_of(message):
        if message == 0:
            return pl.ds(0, 2 * parts)
        if message == 1:
            return pl.ds(2 * parts, extra + later)
        return pl.ds(2 * parts + extra + (message - 1) * later, later)

    def block_copy(message, other, source):
        return pltpu.make_async_remote_copy(
            src_ref=packed.at[other, blocks_of(message)],
            dst_ref=arrived.at[source, blocks_of(message)],
            send_sem=send_sem.at[message, other],
            recv_sem=recv_sem.at[message, source],
            device_id={"date": other},
            device_id_type=pl.DeviceIdType.MESH,
        )

    def send_at(distance, messages):
        for exists, other in at_distance(count, me, distance):
            @pl.when(exists)
            def _():
                for message in messages:
                    block_copy(message, other, me).start()

    def send_all(message):
        for other in others if message >= parts - 1 else reversed(others):
            block_copy(message, other, me).start()

    with jax.named_scope("prepare_first"):
        prepare(0)
    with jax.named_scope("meet_first"):
        pl.semaphore_wait(barrier, greetings)
    if farthest > 1:
        greet(round_sem.at[0])
    send_at(1, [0])
    with jax.named_scope("prepare_rest"):
        for index in range(1, len(chunks)):
            prepare(index)
    send_at(1, [1])
    for distance in range(2, farthest + 1):
        with jax.named_scope("meet_next"):
            pl.semaphore_wait(round_sem.at[distance - 2], greetings)
        if distance < farthest:
            greet(round_sem.at[distance - 1])
        send_at(distance, [0, 1])
    def send_paced(arrived_parts):
        for index, counts in enumerate(SENT):
            first = counts[min(arrived_parts - 1, len(counts) - 1)] if arrived_parts else 2
            messages = range(first, min(counts[min(arrived_parts, len(counts) - 1)], parts + 1))
            if messages:
                @pl.when(core == index)
                def _():
                    for message in messages:
                        send_all(message)

    send_paced(0)
    arrived[me] = packed[me]

    lane = lax.broadcasted_iota(jnp.int32, (2 * dates, LANES), 1)

    def gathered(block):
        return arrived[:, block].reshape(dates, LANES)

    def shared_columns():
        columns = []
        for piece in range(extra):
            both = gathered(2 * parts + piece)
            columns.append((jnp.concatenate([both, pltpu.roll(both, LANES // 2, 1)], axis=0), True))
        return columns

    def span_columns(part, spans):
        columns = []
        for index in spans:
            sides = [
                gathered(later_block(part, side, index) if index else first_block(part, side)) for side in range(2)
            ]
            columns.append((jnp.concatenate(sides, axis=0), False))
        return columns

    def windows_sums(part, columns):
        right = jnp.concatenate([block for block, _ in columns], axis=1)
        for inner in range(QUAD):
            mine = jnp.logical_and(lane < LANES // 2, (lane & (windows - 1)) == part * QUAD + inner)
            own_lane = (lane & (QUAD - 1)) == inner
            left = jnp.concatenate(
                [jnp.where(mine if shared else own_lane, block, jnp.zeros_like(block)) for block, shared in columns],
                axis=1,
            )
            yield cross_sums(left, right)

    def sum_ahead(part):
        for inner, sums in enumerate(windows_sums(part, shared_columns() + span_columns(part, [0]))):
            partial[inner, 0], partial[inner, 1] = sums

    def compute_part(part, ahead):
        with jax.named_scope(f"wait_{part}"):
            for message in range(0 if part == 0 else part + 1, part + 2):
                for other in others:
                    block_copy(message, other, other).wait_recv()
        send_paced(part + 1)
        columns = span_columns(part, range(1, full)) if ahead else shared_columns() + span_columns(part, range(full))
        matrices = []
        for inner, (real_sum, imag_sum) in enumerate(windows_sums(part, columns)):
            window = part * QUAD + inner
            if ahead:
                real_sum, imag_sum = real_sum + partial[inner, 0], imag_sum + partial[inner, 1]
            real, imag = window_coherence(real_sum, imag_sum, looks_count)
            coherence_ref[0, 0, 0, window] = real
            coherence_ref[1, 0, 0, window] = imag
            matrices.append(jnp.concatenate([real, imag], axis=1))
        for inner, (real, imag) in enumerate(link_windows(matrices)):
            vectors[0, pl.ds(part * QUAD + inner, 1)] = real
            vectors[1, pl.ds(part * QUAD + inner, 1)] = imag

    for part in range(parts):
        with jax.named_scope(f"part_{part}"):
            ahead = 0 < part == parts - 1 and full > 1
            if ahead:
                sum_ahead(part)
            compute_part(part, ahead)

    fold, rows, width = own // turned.shape[1], turned.shape[1], 2 * windows
    spread = jnp.concatenate([vectors[0], vectors[1]], axis=0)
    spread = jnp.pad(spread, ((0, LANES - width), (0, 0))).T.reshape(count, fold, rows, LANES)
    folded = spread[:, 0]
    for place in range(1, fold):
        folded = folded + pltpu.roll(
            spread[:, place].reshape(count * rows, LANES), place * width, 1
        ).reshape(count, rows, LANES)
    turned[...] = folded

    def back_copy(other, source):
        return pltpu.make_async_remote_copy(
            src_ref=turned.at[other],
            dst_ref=landed.at[source],
            send_sem=back_send.at[other],
            recv_sem=back_recv.at[source],
            device_id={"date": other},
            device_id_type=pl.DeviceIdType.MESH,
        )

    for other in reversed(others):
        back_copy(other, me).start()
    landed[me] = turned[me]
    with jax.named_scope("wait_back"):
        for other in others:
            back_copy(other, other).wait_recv()
    for side in range(2):
        for place in range(fold):
            first = place * width + side * windows
            linked_ref[side, place * rows : (place + 1) * rows] = jnp.concatenate(
                [landed[source][:, first : first + windows] for source in range(count)], axis=1
            )

    for message in range(parts + 1):
        for other in others:
            block_copy(message, other, me).wait_send()
    for other in others:
        back_copy(other, me).wait_send()


def deliver(coherence_in, linked_in, coherence_out, linked_out, sem):
    copies = [pltpu.make_async_copy(linked_in, linked_out, sem.at[0])]
    windows = coherence_in.shape[3]
    pieces = PIECES if windows % PIECES == 0 else 1
    size = windows // pieces
    for side in range(coherence_in.shape[0]):
        for piece in range(pieces):
            span = pl.ds(piece * size, size)
            copies.append(
                pltpu.make_async_copy(
                    coherence_in.at[side, :, :, span],
                    coherence_out.at[side, :, :, span],
                    sem.at[1 + side * PIECES + piece],
                )
            )
    for copy in copies:
        copy.start()
    for copy in copies:
        copy.wait()


def local(slc, usable):
    looks_count, own_dates, windows = usable.shape
    count = lax.axis_size("date")
    per_device = windows // count
    dates = own_dates * count
    parts = per_device // QUAD
    span = LANES // QUAD
    full = looks_count // span
    extra = pl.cdiv(looks_count - full * span, LANES // per_device // 2)
    fold = max(1, own_dates // 8)
    fold = fold if own_dates % fold == 0 and 2 * per_device * fold <= LANES else 1
    blocks = extra + 2 * full * parts
    results = pl.pallas_call(
        functools.partial(kernel, count, looks_count, per_device),
        out_shape=(
            jax.ShapeDtypeStruct((2, 1, 1, per_device, dates, dates), jnp.bfloat16),
            jax.ShapeDtypeStruct((2, own_dates, windows), jnp.float32),
        ),
        in_specs=[pl.BlockSpec(memory_space=pltpu.HBM)] * 2,
        out_specs=(
            pl.BlockSpec(memory_space=pltpu.VMEM),
            pl.BlockSpec(memory_space=pltpu.VMEM),
        ),
        scratch_shapes=[
            pltpu.VMEM((2, looks_count, own_dates, windows), jnp.bfloat16),
            pltpu.VMEM((looks_count, own_dates, windows), jnp.int32),
            pltpu.VMEM((count, blocks, own_dates, LANES), jnp.bfloat16),
            pltpu.VMEM((count, blocks, own_dates, LANES), jnp.bfloat16),
            pltpu.VMEM((2, per_device, dates), jnp.float32),
            pltpu.VMEM((count, own_dates // fold, LANES), jnp.float32),
            pltpu.VMEM((count, own_dates // fold, LANES), jnp.float32),
            pltpu.SemaphoreType.DMA((full + 1, 2)),
            pltpu.SemaphoreType.DMA((parts + 1, count)),
            pltpu.SemaphoreType.DMA((parts + 1, count)),
            pltpu.SemaphoreType.DMA((count,)),
            pltpu.SemaphoreType.DMA((count,)),
            pltpu.SemaphoreType.REGULAR((count // PAIR + PAIR - 2,)),
            pltpu.VMEM((QUAD, 2, dates, dates), jnp.float32),
        ],
        compiler_params=pltpu.CompilerParams(collective_id=0, has_side_effects=True, vmem_limit_bytes=24 << 20),
    )(pltpu.with_memory_space_constraint(slc, pltpu.HBM), pltpu.with_memory_space_constraint(usable, pltpu.HBM))
    return pl.pallas_call(
        deliver,
        out_shape=tuple(jax.ShapeDtypeStruct(array.shape, array.dtype) for array in results),
        in_specs=[pl.BlockSpec(memory_space=pl.ANY)] * 2,
        out_specs=(pl.BlockSpec(memory_space=pl.ANY),) * 2,
        scratch_shapes=[pltpu.SemaphoreType.DMA((results[0].shape[0] * PIECES + 1,))],
        compiler_params=pltpu.CompilerParams(vmem_limit_bytes=1 << 20),
    )(*results)


def solution(mesh):
    return jax.shard_map(
        local,
        mesh=mesh,
        in_specs=(
            P(None, None, "date", ("slab", "tile", "sub")),
            P(None, "date", ("slab", "tile", "sub")),
        ),
        out_specs=(
            P(None, ("slab", "tile", "sub"), "date", None, None, None),
            P(None, "date", ("slab", "tile", "sub")),
        ),
        check_vma=False,
    )
```
